32 devices in a mesh: ens: 2 (over y), space: 4 (over z), chan: 2 (over x), sub: 2 (over core).
Axes of the slice: x: 2, y: 2, z: 4, core: 2. Of those that a mesh axis runs over, the one named last changes fastest.
Arguments:
- node_state: bfloat16 [8192, 512], P(('ens', 'space'), ('chan', 'sub')), parts along dimension 0, may hold values from -6 to 6
- norm_gains: float32 [2, 512], replicated, may hold values from 0.25 to 1.75
- norm_shifts: float32 [2, 512], replicated, may hold values from -3 to 3
- query_weight: bfloat16 [512, 512], P(None, 'chan')
- key_weight: bfloat16 [512, 512], P(None, 'chan')
- value_weight: bfloat16 [512, 512], P(None, 'chan'), may hold values from -0.25 to 0.25
- out_weight: bfloat16 [512, 512], replicated, may hold values from -0.25 to 0.25
- ffn_in: bfloat16 [2048, 512], P('chan'), may hold values from -0.25 to 0.25
- ffn_out: bfloat16 [2048, 512], P('chan'), may hold values from -0.125 to 0.125
- live_counts: int32 [4], P('space'), may hold values from 512 to 1024, as said below
- send_rows: int32 [4, 2, 256], P('space'), may hold values from 0 to 1023, as said below
- tile_keys: int32 [32, 12], P('space'), may hold values from 0 to 11, as said below
- tile_bits: int32 [32, 12, 4, 128], P('space'), may hold values from -2147483648 to 2147483647, as said below
Outputs:
- updated: bfloat16 [8192, 512], P(('ens', 'space'), ('chan', 'sub')), parts along dimension 0
The draws below stay inside these ranges and needn't reach their ends.
There are 2 independent parts, one for each index of `ens`. The reference program is written for one: setup_inputs(seed, part) draws one part's arguments, and reference() takes and returns one part's arrays. A program takes and returns all parts, laid end to end along the dimension named above; an argument that names none is the same for every part. Nothing has to cross between parts.
Inputs may be any that keep to these rules, and one draw needn't show every extreme that they name: Partition s has live nodes 0 to live_counts[s] - 1; the first and the last partition are full. send_rows[s, 0] lists nodes of partition s read by its lower neighbour, send_rows[s, 1] those read by its upper neighbour; all are live nodes, and entries may repeat. `tile_keys`: slot 0 of every block names the block itself (its index within the partition); other slots name blocks of the same partition (below 8), of the lower halo (from 8) or of the upper halo (from 10); the first partition names no lower halo and the last no upper halo. `tile_bits`: bit j of word w in column r of a slot says whether query r of the block may attend key 32 w + j of the slot's block (bit 31 is the sign bit); in slot 0 every query's own bit is set. Slots whose words are all zero carry no edges.
All inputs are finite; a program needn't handle non-finite values.
Results may differ from the reference program's by a relative error of at most 0.0095.
Values may be sent and summed in bfloat16 or wider, within the bound.
A program may use at most 64 MiB of HBM per device.

```python
import math
import jax
import jax.numpy as jnp
from jax import lax

D = 512
HEADS = 8
HD = 64
FF = 2048
TILE = 128
WORDS = 4
KT = 12
HBLK = 2
HB = 256
NB = 8
NBK = 12
NODE_PART = 1024
NODES = 4096
BLOCKS = 32
N_SPACE = 4


def paired_projection(key):
    shared_part = jax.random.normal(jax.random.fold_in(key, 11), (D, D), jnp.float32) / math.sqrt(D)
    second_part = jax.random.normal(jax.random.fold_in(key, 12), (D, D), jnp.float32) / math.sqrt(D)
    return (shared_part, second_part)


def draw_query_weight(key, part):
    shared_part, second_part = paired_projection(key)
    return shared_part.astype(jnp.bfloat16)


def draw_key_weight(key, part):
    shared_part, second_part = paired_projection(key)
    return second_part.astype(jnp.bfloat16)


def partition_sizes(key):
    parts_total = BLOCKS // NB
    section = jnp.arange(parts_total, dtype=jnp.int32)
    drawn = jax.random.randint(jax.random.fold_in(key, 51), (parts_total,), NODE_PART // 2, NODE_PART + 1, dtype=jnp.int32)
    polar = (section == 0) | (section == parts_total - 1)
    return jnp.where(polar, NODE_PART, drawn)


def draw_live_counts(key, part):
    return partition_sizes(key)


def draw_send_rows(key, part):
    sizes = partition_sizes(key)
    return jax.random.randint(jax.random.fold_in(key, 61), (BLOCKS // NB, 2, HB), 0, sizes[:, None, None], dtype=jnp.int32)


def slot_use(key):
    blocks = jnp.arange(BLOCKS, dtype=jnp.int32)
    section = blocks // NB
    polar = (section == 0) | (section == BLOCKS // NB - 1)
    partial_use = jax.random.randint(jax.random.fold_in(key, 21), (BLOCKS,), (KT + 1) // 2, KT + 1, dtype=jnp.int32)
    return jnp.where(polar, KT, partial_use)


def draw_tile_keys(key, part):
    blocks = jnp.arange(BLOCKS, dtype=jnp.int32)
    local_block = blocks % NB
    section = blocks // NB
    offsets = jax.random.randint(jax.random.fold_in(key, 31), (BLOCKS, KT), 1, NB, dtype=jnp.int32)
    others = (local_block[:, None] + offsets) % NB
    near_low = local_block < NB // 2
    low_pick = NB + jax.random.randint(jax.random.fold_in(key, 32), (BLOCKS,), 0, HBLK, dtype=jnp.int32)
    high_pick = NB + HBLK + jax.random.randint(jax.random.fold_in(key, 33), (BLOCKS,), 0, HBLK, dtype=jnp.int32)
    halo_pick = jnp.where(near_low, low_pick, high_pick)
    outer_side = (section == 0) & near_low | (section == BLOCKS // NB - 1) & jnp.logical_not(near_low)
    second_slot = jnp.where(outer_side, others[:, 1], halo_pick)
    return jnp.concatenate([local_block[:, None], second_slot[:, None], others[:, 2:]], axis=1)


def draw_tile_bits(key, part):
    random_words = jax.random.randint(jax.random.fold_in(key, 41), (BLOCKS, KT, WORDS, TILE), -2147483647, 2147483647, dtype=jnp.int32)
    slot_live = (jnp.arange(KT, dtype=jnp.int32)[None, :] < slot_use(key)[:, None]).astype(jnp.int32)
    random_words = random_words * slot_live[:, :, None, None]
    rows_at = jnp.arange(TILE, dtype=jnp.int32)
    own_word = jnp.arange(WORDS, dtype=jnp.int32)[:, None] == (rows_at // 32)[None, :]
    diagonal = jnp.where(own_word, jnp.left_shift(jnp.int32(1), rows_at % 32)[None, :], jnp.int32(0))
    first_slot = jnp.bitwise_or(random_words[:, :1], diagonal[None, None])
    return jnp.concatenate([first_slot, random_words[:, 1:]], axis=1)


def block_levels(key, dims, cuts, smallest, top_value):
    factor_of = 1.0
    for dim, shards_of in cuts:
        draws = jax.random.uniform(jax.random.fold_in(jax.random.fold_in(key, 6), dim), (shards_of,), jnp.float32, smallest / len(cuts), top_value / len(cuts))
        factor_of = factor_of * jnp.repeat(jnp.exp(draws), dims[dim] // shards_of).reshape((-1,) + (1,) * (len(dims) - 1 - dim))
    return factor_of


def bell_draw(rng, shape, width, bound, shards=(), kind=jnp.bfloat16):
    values = jax.random.normal(rng, shape, jnp.float32) * width
    if len(shards) > 0:
        values = block_levels(rng, shape, shards, -0.22, 0.18) * values
    return jnp.clip(values, min=-bound, max=bound).astype(kind)


def setup_inputs(seed: int = 0, part: int = 0) -> dict:
    streams_of = jax.random.split(jax.random.key(seed), 14)
    own_keys = jax.random.split(jax.random.fold_in(streams_of[13], part), 14)
    return {
        "node_state": bell_draw(own_keys[0], (NODES, D), 1.0, 6.0, ((0, 4), (1, 4))),
        "norm_gains": jnp.clip(1.0 + 0.15 * jax.random.normal(streams_of[1], (2, D), jnp.float32), 0.25, 1.75),
        "norm_shifts": bell_draw(streams_of[2], (2, D), 0.5, 3.0, (), jnp.float32),
        "query_weight": draw_query_weight(jax.random.fold_in(streams_of[13], 71), part),
        "key_weight": draw_key_weight(jax.random.fold_in(streams_of[13], 71), part),
        "value_weight": bell_draw(streams_of[5], (D, D), D ** -0.5, 0.25, ((1, 2),)),
        "out_weight": bell_draw(streams_of[6], (D, D), D ** -0.5, 0.25),
        "ffn_in": bell_draw(streams_of[7], (FF, D), D ** -0.5, 0.25, ((0, 2),)),
        "ffn_out": bell_draw(streams_of[8], (FF, D), FF ** -0.5, 0.125, ((0, 2),)),
        "live_counts": draw_live_counts(jax.random.fold_in(streams_of[13], 71), part),
        "send_rows": draw_send_rows(jax.random.fold_in(streams_of[13], 71), part),
        "tile_keys": draw_tile_keys(jax.random.fold_in(streams_of[13], 71), part),
        "tile_bits": draw_tile_bits(jax.random.fold_in(streams_of[13], 71), part),
    }


NORM_EPS = 1e-05
NEG_FILL = -1e+30

def normalize_rows(source, gain_row, shift_row):
    row_mean = lax.optimization_barrier(jnp.mean(source, axis=-1, keepdims=True))
    spread = lax.optimization_barrier(jnp.mean(source * source, axis=-1, keepdims=True)) - row_mean * row_mean
    return (source - row_mean) * lax.rsqrt(spread + NORM_EPS) * gain_row + shift_row

def unpack_allowed(key_bits, key_ids, live_count, tile_size, blocks_own):
    shifts = jnp.arange(32, dtype=jnp.int32)
    expanded = jnp.right_shift(key_bits[..., None, :], shifts[:, None]) & 1
    lead_shape = key_bits.shape[:-2]
    expanded = expanded.reshape(lead_shape + (tile_size, tile_size))
    key_index = key_ids[..., None] * tile_size + jnp.arange(tile_size, dtype=jnp.int32)
    key_live = (key_ids[..., None] >= blocks_own) | (key_index < live_count)
    slot_count = key_ids.shape[-1]
    slot_first = jnp.arange(slot_count, dtype=jnp.int32)[:, None, None] == 0
    diagonal = jnp.arange(tile_size, dtype=jnp.int32)[:, None] == jnp.arange(tile_size, dtype=jnp.int32)[None, :]
    own_bit = slot_first & diagonal[None]
    return (expanded == 1) & (key_live[..., None] | own_bit)

def reference(node_state, norm_gains, norm_shifts, query_weight, key_weight, value_weight, out_weight, ffn_in, ffn_out, live_counts, send_rows, tile_keys, tile_bits):
    float_state = node_state.astype(jnp.float32)
    normed = normalize_rows(float_state, norm_gains[0], norm_shifts[0]).astype(jnp.bfloat16)
    queries = jnp.dot(normed, query_weight, preferred_element_type=jnp.float32).astype(jnp.bfloat16)
    key_rows = jnp.dot(normed, key_weight, preferred_element_type=jnp.float32).astype(jnp.bfloat16)
    value_rows = jnp.dot(normed, value_weight, preferred_element_type=jnp.float32).astype(jnp.bfloat16)
    key_values = jnp.concatenate([key_rows, value_rows], axis=1).reshape(N_SPACE, NODE_PART, 2 * D)
    upward = jnp.take_along_axis(key_values, send_rows[:, 1, :, None], axis=1)
    downward = jnp.take_along_axis(key_values, send_rows[:, 0, :, None], axis=1)
    empty_rim = jnp.zeros((1, HB, 2 * D), key_values.dtype)
    lower_rim = jnp.concatenate([empty_rim, upward[:-1]], axis=0)
    upper_rim = jnp.concatenate([downward[1:], empty_rim], axis=0)
    extended = jnp.concatenate([key_values, lower_rim, upper_rim], axis=1).reshape(N_SPACE, NBK, TILE, 2 * D)
    query_blocks = queries.reshape(N_SPACE, NB, TILE, HEADS, HD)
    key_ids = tile_keys.reshape(N_SPACE, NB, KT)
    key_bits = tile_bits.reshape(N_SPACE, NB, KT, WORDS, TILE)
    score_scale = 1.0 / math.sqrt(HD)

    def one_partition(inputs):
        ext_part, q_part, id_part, bit_part, count_part = inputs
        chosen = ext_part[id_part]
        keys_part = chosen[..., :D].reshape(NB, KT, TILE, HEADS, HD).astype(jnp.float32)
        values_part = chosen[..., D:].reshape(NB, KT, TILE, HEADS, HD).astype(jnp.float32)
        scores = jnp.einsum('brhd,btkhd->bhrtk', q_part.astype(jnp.float32), keys_part) * score_scale
        allowed = unpack_allowed(bit_part, id_part, count_part, TILE, NB)
        allowed = jnp.transpose(allowed, (0, 3, 1, 2))[:, None]
        masked = jnp.where(allowed, scores, NEG_FILL)
        row_max = lax.optimization_barrier(jnp.max(masked, axis=(3, 4), keepdims=True))
        weights = jnp.where(allowed, jnp.exp(scores - row_max), 0.0)
        row_total = lax.optimization_barrier(jnp.sum(weights, axis=(3, 4)))
        rounded = lax.optimization_barrier(weights.astype(jnp.bfloat16)).astype(jnp.float32)
        mixed_heads = jnp.einsum('bhrtk,btkhd->brhd', rounded, values_part)
        mixed_heads = mixed_heads / jnp.transpose(row_total, (0, 2, 1))[..., None]
        return mixed_heads.astype(jnp.bfloat16).reshape(NB * TILE, D)
    attended = lax.map(one_partition, (extended, query_blocks, key_ids, key_bits, live_counts)).reshape(NODES, D)
    after_attn = float_state + jnp.dot(attended, out_weight, preferred_element_type=jnp.float32)
    normed_two = normalize_rows(after_attn, norm_gains[1], norm_shifts[1]).astype(jnp.bfloat16)
    hidden = jax.nn.gelu(jnp.dot(normed_two, ffn_in.T, preferred_element_type=jnp.float32)).astype(jnp.bfloat16)
    result = after_attn + jnp.dot(hidden, ffn_out, preferred_element_type=jnp.float32)
    node_at = jnp.arange(NODES, dtype=jnp.int32)
    node_live = node_at % NODE_PART < live_counts[node_at // NODE_PART]
    return jnp.where(node_live[:, None], result, 0.0).astype(jnp.bfloat16)
```

```python
import math

import jax
import jax.numpy as jnp
from jax import lax
from jax.experimental import pallas as pl
from jax.experimental.pallas import tpu as pltpu
from jax.sharding import PartitionSpec as P

HD = 64


NORM_EPS = 1e-05
NEG_FILL = -1e30


def padded_2(array, sides, width):
    for axis, dim in sides:
        size, length = (lax.axis_size(axis), array.shape[dim])
        up = [(i, (i + 1) % size) for i in range(size - 1)]
        down = [(j, i) for i, j in up]
        last = lax.slice_in_dim(array, length - width, length, axis=dim)
        leading = lax.slice_in_dim(array, 0, width, axis=dim)
        before = lax.ppermute(last, axis, up)
        after = lax.ppermute(leading, axis, down)
        array = jnp.concatenate([before, array, after], axis=dim)
    return array


def normalize_rows(source, gain_row, shift_row):
    row_mean = jnp.mean(source, axis=-1, keepdims=True)
    spread = jnp.mean(source * source, axis=-1, keepdims=True) - row_mean * row_mean
    return (source - row_mean) * lax.rsqrt(spread + NORM_EPS) * gain_row + shift_row


def unpack_allowed(key_bits, key_ids, live_count, tile_size, blocks_own):
    shifts = jnp.arange(32, dtype=jnp.int32)
    expanded = jnp.right_shift(key_bits[..., None, :], shifts[:, None]) & 1
    lead_shape = key_bits.shape[:-2]
    expanded = expanded.reshape(lead_shape + (tile_size, tile_size))
    key_index = key_ids[..., None] * tile_size + jnp.arange(tile_size, dtype=jnp.int32)
    key_live = (key_ids[..., None] >= blocks_own) | (key_index < live_count)
    slot_count = key_ids.shape[-1]
    slot_first = jnp.arange(slot_count, dtype=jnp.int32)[:, None, None] == 0
    diagonal = (
        jnp.arange(tile_size, dtype=jnp.int32)[:, None]
        == jnp.arange(tile_size, dtype=jnp.int32)[None, :]
    )
    own_bit = slot_first & diagonal[None]
    return (expanded == 1) & (key_live[..., None] | own_bit)


def hidden_term(rows, in_piece, out_piece):
    hidden = jax.nn.gelu(
        lax.dot_general(
            rows, in_piece, (((1,), (1,)), ((), ())), preferred_element_type=jnp.float32
        )
    ).astype(jnp.bfloat16)
    return jnp.dot(hidden, out_piece, preferred_element_type=jnp.float32)


def on_device(
    node_state,
    norm_gains,
    norm_shifts,
    query_weight,
    key_weight,
    value_weight,
    out_weight,
    ffn_in,
    ffn_out,
    live_counts,
    send_rows,
    tile_keys,
    tile_bits,
):
    n_chan = lax.axis_size("chan")
    n_sub = lax.axis_size("sub")
    groups = n_chan * n_sub
    chan_at = lax.axis_index("chan")
    sub_at = lax.axis_index("sub")
    node_rank = chan_at * n_sub + sub_at
    node_count = node_state.shape[0]
    tile_size = tile_bits.shape[-1]
    word_count = tile_bits.shape[-2]
    slot_count = tile_keys.shape[1]
    blocks_own = tile_keys.shape[0]
    per_rank = node_count // groups
    head_cols = query_weight.shape[1]
    heads_here = head_cols // HD
    halo_rows = send_rows.shape[-1]
    live_count = live_counts[0]

    def own_half(source):
        step_rows = source.shape[0] // groups
        shaped = source.reshape((n_chan, n_sub, step_rows) + source.shape[1:])
        picked = lax.dynamic_index_in_dim(shaped, sub_at, 1, keepdims=False)
        return picked.reshape((n_chan * step_rows,) + source.shape[1:])

    node_rows = lax.all_to_all(node_state, ("chan", "sub"), split_axis=0, concat_axis=1, tiled=True)
    pair_weight = jnp.concatenate([key_weight, value_weight], axis=1)
    gathered = lax.all_gather(node_state, ("chan", "sub"), axis=1, tiled=True)
    normed = normalize_rows(gathered.astype(jnp.float32), norm_gains[0], norm_shifts[0]).astype(
        jnp.bfloat16
    )
    key_values = jnp.dot(normed, pair_weight, preferred_element_type=jnp.float32).astype(
        jnp.bfloat16
    )
    queries = jnp.dot(own_half(normed), query_weight, preferred_element_type=jnp.float32).astype(
        jnp.bfloat16
    )
    send_list = send_rows.reshape(2 * halo_rows)
    outgoing = jnp.take(key_values, send_list, axis=0)
    padded = padded_2(outgoing, (("space", 0),), halo_rows)
    extended = jnp.concatenate([key_values, padded[:halo_rows], padded[-halo_rows:]], axis=0)
    key_blocks = extended.reshape(-1, tile_size, 2 * head_cols)
    key_ids = own_half(tile_keys)
    key_bits = own_half(tile_bits)
    block_total = key_ids.shape[0]
    per_round = math.gcd(block_total, 4)
    rounds = block_total // per_round
    score_scale = 1.0 / math.sqrt(HD)

    def attend(inputs):
        q_part, id_part, bit_part = inputs
        chosen = key_blocks[id_part]
        keys_part = chosen[..., :head_cols].reshape(
            per_round, slot_count, tile_size, heads_here, HD
        )
        values_part = chosen[..., head_cols:].reshape(
            per_round, slot_count, tile_size, heads_here, HD
        )
        scores = (
            jnp.einsum("grhd,gtkhd->ghrtk", q_part, keys_part, preferred_element_type=jnp.float32)
            * score_scale
        )
        allowed = unpack_allowed(bit_part, id_part, live_count, tile_size, blocks_own)
        allowed = jnp.transpose(allowed, (0, 3, 1, 2))[:, None]
        masked = jnp.where(allowed, scores, NEG_FILL)
        row_max = jnp.max(masked, axis=(3, 4), keepdims=True)
        weights = jnp.where(allowed, jnp.exp(scores - row_max), 0.0)
        row_total = jnp.sum(weights, axis=(3, 4))
        mixed_heads = jnp.einsum(
            "ghrtk,gtkhd->grhd",
            weights.astype(jnp.bfloat16),
            values_part,
            preferred_element_type=jnp.float32,
        )
        mixed_heads = mixed_heads / jnp.transpose(row_total, (0, 2, 1))[..., None]
        return mixed_heads.astype(jnp.bfloat16).reshape(per_round * tile_size, head_cols)

    query_groups = queries.reshape(rounds, per_round, tile_size, heads_here, HD)
    attended = lax.map(
        attend,
        (
            query_groups,
            key_ids.reshape(rounds, per_round, slot_count),
            key_bits.reshape(rounds, per_round, slot_count, word_count, tile_size),
        ),
    )
    mixed_rows = jnp.dot(
        lax.all_to_all(
            attended.reshape(n_chan, per_rank, head_cols),
            "chan",
            split_axis=0,
            concat_axis=2,
            tiled=True,
        )[0],
        out_weight,
        preferred_element_type=jnp.float32,
    )
    after_attn = node_rows.astype(jnp.float32) + mixed_rows
    normed_two = normalize_rows(after_attn, norm_gains[1], norm_shifts[1]).astype(jnp.bfloat16)
    all_rows = lax.all_gather(normed_two, "chan", axis=0, tiled=True)
    update = lax.psum_scatter(
        hidden_term(all_rows, ffn_in, ffn_out).astype(jnp.bfloat16),
        "chan",
        scatter_dimension=0,
        tiled=True,
    ).astype(jnp.float32)
    position = node_rank * per_rank + jnp.arange(per_rank, dtype=jnp.int32)
    result = jnp.where((position < live_count)[:, None], after_attn + update, 0.0).astype(
        jnp.bfloat16
    )
    return lax.all_to_all(result, ("chan", "sub"), split_axis=1, concat_axis=0, tiled=True)


MESH = pl.DeviceIdType.MESH
LOG2E = 1.4426950408889634
NT = (((1,), (1,)), ((), ()))


def gelu_tanh(u):
    inner = 0.7978845608028654 * (u + 0.044715 * (u * u * u))
    return 0.5 * u * (1.0 + jnp.tanh(inner))


def layer_kernel(
    x_hbm,
    gains_hbm,
    shifts_hbm,
    wq_hbm,
    wk_hbm,
    wv_hbm,
    wo_hbm,
    fin_hbm,
    fout_hbm,
    live_hbm,
    send_hbm,
    tk_hbm,
    bits_hbm,
    out_ref,
    xq,
    gx,
    hsend,
    kv,
    wvt,
    qbuf,
    bias_ref,
    s_ref,
    att,
    full_part,
    half_part,
    from_sib,
    from_x,
    proj_w,
    ffn_w,
    norm_ref,
    send_ref,
    bits_ref,
    live_ref,
    tk_ref,
    w_sem,
    loc_sem,
    a_send,
    a_recv,
    x_send,
    x_recv,
    z_send,
    z_recv,
    h_send,
    h_recv,
    k_send,
    k_recv,
    t_send,
    t_recv,
    p_send,
    p_recv,
    d_send,
    d_recv,
):
    f32, bf16 = jnp.float32, jnp.bfloat16
    rows, cols = x_hbm.shape
    groups = gx.shape[0]
    tile = bits_hbm.shape[-1]
    words = bits_hbm.shape[-2]
    slots = tk_ref.shape[1]
    blocks_own = tk_ref.shape[0]
    halo = send_hbm.shape[-1]
    width, head_cols = wv_hbm.shape
    hidden_here = fin_hbm.shape[0]
    pw = 2 * HD
    pairs = head_cols // pw
    half = rows // 2
    n_here = half // tile
    n_halo = halo // tile

    c = lax.axis_index("chan")
    s = lax.axis_index("sub")
    z = lax.axis_index("space")
    nz = lax.axis_size("space")
    own = c * 2 + s
    sib = c * 2 + 1 - s
    far = (1 - c) * 2
    xdev = {"chan": 1 - c}
    sdev = {"sub": 1 - s}
    has_up = z < nz - 1
    has_down = z > 0
    has_halo = jnp.where(s == 0, z, nz - 1 - z) > 0

    own_half = pl.ds(pl.multiple_of(s * half, half), half)
    sib_half = pl.ds(pl.multiple_of((1 - s) * half, half), half)
    local = pltpu.make_async_copy(x_hbm, xq, loc_sem.at[0])
    local_own = pltpu.make_async_copy(x_hbm.at[own_half], gx.at[own, pl.ds(0, half)], loc_sem.at[1])
    fin = ffn_w.at[pl.ds(0, hidden_here)]
    fout = ffn_w.at[pl.ds(hidden_here, hidden_here)]
    wo = ffn_w.at[pl.ds(2 * hidden_here, width)]
    n_norms = gains_hbm.shape[0]
    loads = (
        (send_hbm, send_ref, 0),
        (tk_hbm, tk_ref, 1),
        (live_hbm, live_ref, 2),
        (bits_hbm, bits_ref, 3),
        (wv_hbm, proj_w.at[:, pl.ds(2 * head_cols, head_cols)], 4),
        (gains_hbm, norm_ref.at[pl.ds(0, n_norms)], 5),
        (shifts_hbm, norm_ref.at[pl.ds(n_norms, n_norms)], 5),
        (wk_hbm, proj_w.at[:, pl.ds(0, head_cols)], 4),
        (wq_hbm, proj_w.at[:, pl.ds(head_cols, head_cols)], 4),
        (wo_hbm, wo, 6),
        (fin_hbm, fin, 6),
        (fout_hbm, fout, 6),
    )
    landed = (send_ref, tk_ref, live_ref, bits_ref, proj_w, norm_ref, ffn_w)

    def loaded(i):
        pltpu.make_async_copy(landed[i], landed[i], w_sem.at[i]).wait()


    barrier = pltpu.get_barrier_semaphore()

    def greet(dev):
        pl.semaphore_signal(barrier, inc=1, device_id=dev, device_id_type=MESH)

    greet(xdev)
    greet({"chan": 1 - c, "sub": 1 - s})
    greet(sdev)

    @pl.when(has_up)
    def _():
        greet({"space": z + 1})
        greet({"space": z + 1, "sub": 1 - s})

    @pl.when(has_down)
    def _():
        greet({"space": z - 1})
        greet({"space": z - 1, "sub": 1 - s})

    local.start()
    local_own.start()
    for a, b, i in loads:
        pltpu.make_async_copy(a, b, w_sem.at[i]).start()
    with jax.named_scope("barrierw"):
        pl.semaphore_wait(barrier, 3 + jnp.where(has_up, 2, 0) + jnp.where(has_down, 2, 0))
        local.wait()

    def rdma(src, dst, ss, rs, dev):
        return pltpu.make_async_remote_copy(
            src_ref=src, dst_ref=dst, send_sem=ss, recv_sem=rs, device_id=dev, device_id_type=MESH
        )

    def block(i):
        return pl.ds(pl.multiple_of(i * tile, tile), tile)

    def a_copy():
        return rdma(xq.at[sib_half], gx.at[own, pl.ds(0, half)], a_send, a_recv, sdev)

    def a_wait():
        part = gx.at[sib, pl.ds(0, half)]
        rdma(part, part, a_send, a_recv, sdev).wait_recv()

    def x_copy(i, to):
        src = xq.at[pl.ds(to * half + i * tile, tile)]
        dev = {"chan": 1 - c, "sub": to}
        return rdma(src, gx.at[own, block(i)], x_send, x_recv.at[i], dev)

    def x_wait(i):
        part = gx.at[pl.ds(far, 2), block(i)]
        rdma(part, part, x_send, x_recv.at[i], xdev).wait_recv()

    halo_at = pl.ds(half, halo)

    def z_copy(side):
        if side == 1:
            dev = {"space": z + 1, "sub": 0}
        else:
            dev = {"space": z - 1, "sub": 1}
        return rdma(hsend.at[side], gx.at[own, halo_at], z_send.at[side], z_recv, dev)

    def z_wait():
        part = gx.at[pl.ds(c * 2, 2), halo_at]
        rdma(part, part, z_send.at[0], z_recv, sdev).wait_recv()

    def h_copy(k):
        part = gx.at[pl.ds(c * 2, 2), pl.ds(half + k * tile, tile)]
        return rdma(part, part, h_send, h_recv.at[k], xdev)

    def h_wait(k):
        part = gx.at[pl.ds(far, 2), pl.ds(half + k * tile, tile)]
        rdma(part, part, h_send, h_recv.at[k], xdev).wait_recv()

    for i in range(n_here):
        x_copy(i, 0).start()
        x_copy(i, 1).start()
    a_copy().start()
    loaded(0)

    with jax.named_scope("onehot"):
        lanes = lax.broadcasted_iota(jnp.int32, (halo, tile), 1)
        for side in range(2):
            wanted = jnp.broadcast_to(send_ref[0, side : side + 1, :], (tile, halo)).T
            picks = jnp.concatenate(
                [(wanted == lanes + k * tile).astype(f32).astype(bf16) for k in range(rows // tile)],
                axis=1,
            )
            hsend[side] = jnp.dot(picks, xq[...], preferred_element_type=f32).astype(bf16)

    @pl.when(has_up)
    def _():
        z_copy(1).start()

    @pl.when(has_down)
    def _():
        z_copy(0).start()

    @pl.when(jnp.logical_not(has_halo))
    def _():
        gx[:, halo_at, :] = jnp.zeros((groups, halo, cols), bf16)

    for i in range(1, 5):
        loaded(i)
    wvt[...] = proj_w[:, 2 * head_cols :].astype(f32).T.astype(bf16)

    live = live_ref[0]
    word_rows = tile // words
    row_id = lax.broadcasted_iota(jnp.int32, (tile, tile), 0)
    col_id = lax.broadcasted_iota(jnp.int32, (tile, tile), 1)
    shifts = lax.broadcasted_iota(jnp.int32, (word_rows, tile), 0)
    low_half = lax.broadcasted_iota(jnp.int32, (tile, pw), 1) < HD

    def mask_block(j, carry):
        b = s * n_here + j
        for t in range(slots):
            slot_id = tk_ref[b, t]
            block_bits = bits_ref[b, t]
            set_bits = jnp.concatenate(
                [
                    jnp.right_shift(
                        jnp.broadcast_to(block_bits[w : w + 1, :], (word_rows, tile)), shifts
                    )
                    & 1
                    for w in range(words)
                ],
                axis=0,
            )
            limit = jnp.where(slot_id >= blocks_own, tile, live - slot_id * tile)
            good = row_id < limit
            if t == 0:
                good = good | (row_id == col_id)
            bias_ref[j, t * tile : (t + 1) * tile] = jnp.where(
                (set_bits == 1) & good, 0.0, NEG_FILL
            )
        return carry

    with jax.named_scope("mask"):
        lax.fori_loop(0, n_here, mask_block, 0)

    def full_rows(at):
        return jnp.concatenate([gx[g, at] for g in range(groups)], axis=1).astype(f32)

    def norm(v, which):
        mean = jnp.mean(v, axis=-1, keepdims=True)
        spread = jnp.mean(v * v, axis=-1, keepdims=True) - mean * mean
        scaled = (v - mean) * lax.rsqrt(spread + NORM_EPS)
        gain, shift = norm_ref[which : which + 1, :], norm_ref[n_norms + which : n_norms + which + 1, :]
        return scaled * gain + shift

    scale = LOG2E / math.sqrt(HD)

    per_core = n_here + n_halo

    def k_copy(core, i):
        part = kv.at[core * per_core + i]
        return rdma(part, part, k_send.at[0], k_recv.at[i], sdev)

    def project(i, with_queries):
        normed = norm(full_rows(block(i)), 0).astype(bf16)
        to = s * per_core + i
        wanted = (2 if with_queries else 1) * head_cols
        both = jnp.dot(normed, proj_w[:, :wanted], preferred_element_type=f32)
        for pair in range(pairs):
            kv[to, pair] = both[:, pair * pw : (pair + 1) * pw].astype(bf16)
        if with_queries:
            qbuf[block(i)] = (both[:, head_cols:] * scale).astype(bf16)
        values = lax.dot_general(wvt[...], normed, NT, preferred_element_type=f32)
        for pair in range(pairs):
            kv[to, pairs + pair] = values[pair * pw : (pair + 1) * pw].astype(bf16)
        k_copy(s, i).start()

    loaded(5)
    local_own.wait()
    with jax.named_scope("aw"):
        a_wait()

    def own_step(i, carry):
        with jax.named_scope("xw"):
            x_wait(i)
        with jax.named_scope("proj"):
            project(i, True)
        return carry

    early = n_here // 2
    lax.fori_loop(0, early, own_step, 0)

    with jax.named_scope("zw"):

        @pl.when(has_halo)
        def _():
            z_wait()
            for k in range(n_halo):
                h_copy(k).start()

    lax.fori_loop(early, n_here, own_step, 0)
    for k in range(n_halo):
        with jax.named_scope("hw"):

            @pl.when(has_halo)
            def _():
                h_wait(k)

        with jax.named_scope("hproj"):
            project(n_here + k, False)

    with jax.named_scope("kvw"):
        for i in range(n_here + n_halo):
            k_copy(1 - s, i).wait_recv()

    def t_copy(j):
        part = att.at[pl.ds(c * pairs, pairs), block(j)]
        return rdma(part, part, t_send, t_recv.at[j], xdev)

    def t_wait(j):
        part = att.at[pl.ds((1 - c) * pairs, pairs), block(j)]
        rdma(part, part, t_send, t_recv.at[j], xdev).wait_recv()

    def stored(block_id):
        halo_id = block_id - blocks_own
        in_own = block_id // n_here * per_core + block_id % n_here
        in_halo = halo_id // n_halo * per_core + n_here + halo_id % n_halo
        return jnp.where(block_id < blocks_own, in_own, in_halo)

    ones = jnp.ones((16, 2 * tile), bf16)
    span = 1

    def attend_block(j, carry):
        b = s * n_here + j
        ids = [stored(tk_ref[b, t]) for t in range(slots)]
        q_rows = qbuf[block(j)]
        for pair in range(pairs):
            at = slice(pair * pw, (pair + 1) * pw)
            q_pair = q_rows[:, at]
            zero = jnp.zeros_like(q_pair)
            wide = jnp.concatenate(
                [jnp.where(low_half, q_pair, zero), jnp.where(low_half, zero, q_pair)], axis=0
            )
            top = jnp.full((8, 2 * tile), NEG_FILL, f32)
            for t in range(0, slots, span):
                lot = slice(t * tile, (t + span) * tile)
                keys = jnp.concatenate([kv[ids[t + u], pair] for u in range(span)], axis=0)
                bias = bias_ref[j, lot]
                scores = lax.dot_general(keys, wide, NT, preferred_element_type=f32)
                scores = scores + jnp.concatenate([bias, bias], axis=1)
                s_ref[pair, lot] = scores
                top = jnp.maximum(
                    top, jnp.max(scores.reshape(span * tile // 8, 8, 2 * tile), axis=0)
                )
            top = jnp.max(top, axis=0, keepdims=True)
            mixed = jnp.zeros((pw + 16, 2 * tile), f32)
            for t in range(0, slots, 2):
                p = jnp.exp2(s_ref[pair, t * tile : (t + 2) * tile] - top).astype(bf16)
                values = jnp.concatenate(
                    [kv[ids[t], pairs + pair], kv[ids[t + 1], pairs + pair]], axis=1
                )
                values = jnp.concatenate([values, ones], axis=0)
                mixed = mixed + jnp.dot(values, p, preferred_element_type=f32)
            inverse = 1.0 / mixed[pw : pw + 1]
            pieces = [
                mixed[:HD, :tile] * inverse[:, :tile],
                mixed[HD:pw, tile:] * inverse[:, tile:],
            ]
            att[c * pairs + pair, block(j)] = jnp.concatenate(pieces, axis=0).T.astype(bf16)
        t_copy(j).start()
        return carry

    with jax.named_scope("attend"):
        lax.fori_loop(0, n_here, attend_block, 0)

    loaded(6)

    def p_copy(j, to):
        src = half_part.at[j, far + to]
        dev = {"chan": 1 - c, "sub": to}
        return rdma(src, from_x.at[j, s], p_send, p_recv.at[j], dev)

    def p_wait(j):
        part = from_x.at[j]
        rdma(part, part, p_send, p_recv.at[j], xdev).wait_recv()

    def d_copy(j):
        return rdma(full_part.at[j, sib], from_sib.at[j], d_send, d_recv.at[j], sdev)

    def ffn_block(j, carry):
        with jax.named_scope("tw"):
            t_wait(j)
        at = block(j)
        mixed = jnp.concatenate([att[g, at] for g in range(2 * pairs)], axis=1)
        after = full_rows(at) + jnp.dot(mixed, wo[...], preferred_element_type=f32)
        normed_two = norm(after, 1).astype(bf16)
        hidden = gelu_tanh(
            lax.dot_general(normed_two, fin[...], NT, preferred_element_type=f32)
        ).astype(bf16)
        part = jnp.dot(hidden, fout[...], preferred_element_type=f32)
        for g in range(groups):
            half_part[j, g] = part[:, g * cols : (g + 1) * cols].astype(bf16)
        p_copy(j, 0).start()
        p_copy(j, 1).start()
        whole = part + after
        for g in range(groups):
            full_part[j, g] = whole[:, g * cols : (g + 1) * cols]
        d_copy(j).start()
        return carry

    with jax.named_scope("ffn"):
        lax.fori_loop(0, n_here, ffn_block, 0)

    in_block = lax.broadcasted_iota(jnp.int32, (tile, cols), 0)

    def finish(j, carry):
        with jax.named_scope("pw"):
            d_copy(j).wait_recv()
            p_wait(j)
        for core, kept in ((s, full_part[j, own]), (1 - s, from_sib[j])):
            base = core * half + j * tile
            summed = kept + from_x[j, core].astype(f32)
            done = jnp.where(base + in_block < live, summed, 0.0).astype(bf16)
            out_ref[pl.ds(pl.multiple_of(base, tile), tile)] = done
        return carry

    with jax.named_scope("finish"):
        lax.fori_loop(0, n_here, finish, 0)

    def sent(part, sem):
        rdma(part, part, sem, sem, sdev).wait_send()

    with jax.named_scope("endw"):
        sent(xq, x_send)
        sent(xq.at[own_half], a_send)
        sent(kv.at[pl.ds(s * per_core, per_core)], k_send.at[0])
        sent(att.at[pl.ds(c * pairs, pairs)], t_send)
        sent(half_part.at[:, pl.ds(far, 2)], p_send)
        sent(from_sib, d_send)

        @pl.when(has_up)
        def _():
            z_copy(1).wait_send()

        @pl.when(has_down)
        def _():
            z_copy(0).wait_send()

        @pl.when(has_halo)
        def _():
            sent(gx.at[pl.ds(c * 2, 2), halo_at], h_send)


def one_kernel(*args):
    (x, gains, shifts, wq, wk, wv, wo, fin, fout, live, send, tk, bits) = args
    f32, bf16 = jnp.float32, jnp.bfloat16
    rows, cols = x.shape
    width = gains.shape[1]
    groups = lax.axis_size("chan") * lax.axis_size("sub")
    halo = send.shape[-1]
    tile = bits.shape[-1]
    slots = tk.shape[1]
    ext = rows + 2 * halo
    head_cols = wq.shape[1]
    half = rows // 2
    pairs = head_cols // (2 * HD)
    n_here = half // tile
    n_halo = halo // tile
    vmem = pltpu.VMEM
    dma = pltpu.SemaphoreType.DMA
    in_any = pl.BlockSpec(memory_space=pl.ANY)
    return pl.pallas_call(
        layer_kernel,
        out_shape=pltpu.VMEM(x.shape, bf16),
        in_specs=[in_any] * 13,
        out_specs=pl.BlockSpec(memory_space=pltpu.VMEM),
        scratch_shapes=[
            vmem(x.shape, bf16),
            vmem((groups, half + halo, cols), bf16),
            vmem((2, halo, cols), bf16),
            vmem((ext // tile, 2 * pairs, tile, 2 * HD), bf16),
            vmem((head_cols, width), bf16),
            vmem((half, head_cols), bf16),
            vmem((n_here, slots * tile, tile), f32),
            vmem((pairs, slots * tile, 2 * tile), f32),
            vmem((2 * pairs, half, 2 * HD), bf16),
            vmem((n_here, groups, tile, cols), f32),
            vmem((n_here, groups, tile, cols), bf16),
            vmem((n_here, tile, cols), f32),
            vmem((n_here, 2, tile, cols), bf16),
            vmem((width, 3 * head_cols), bf16),
            vmem((2 * fin.shape[0] + wo.shape[0], width), bf16),
            vmem((2 * gains.shape[0], width), f32),
            vmem(send.shape, jnp.int32),
            vmem(bits.shape, jnp.int32),
            pltpu.SMEM(live.shape, jnp.int32),
            pltpu.SMEM(tk.shape, jnp.int32),
            dma((7,)),
            dma((2,)),
            dma,
            dma,
            dma,
            dma((n_here,)),
            dma((2,)),
            dma,
            dma,
            dma((n_halo,)),
            dma((1,)),
            dma((n_here + n_halo,)),
            dma,
            dma((n_here,)),
            dma,
            dma((n_here,)),
            dma,
            dma((n_here,)),
        ],
        compiler_params=pltpu.CompilerParams(collective_id=0, has_side_effects=True),
    )(*args)


def on_any_device(*args):
    two_by_two = lax.axis_size("chan") == 2 and lax.axis_size("sub") == 2
    cols, head_cols = args[0].shape[1], args[3].shape[1]
    tile, halo = args[12].shape[-1], args[10].shape[-1]
    rows_fit = args[0].shape[0] % (4 * tile) == 0 and halo % (2 * tile) == 0
    if two_by_two and cols % 128 == 0 and head_cols % (2 * HD) == 0 and rows_fit and args[11].shape[1] % 2 == 0:
        return one_kernel(*args)
    return on_device(*args)


def solution(mesh):
    in_specs = (
        P(("ens", "space"), ("chan", "sub")),
        P(),
        P(),
        P(None, "chan"),
        P(None, "chan"),
        P(None, "chan"),
        P(),
        P("chan", None),
        P("chan", None),
        P("space"),
        P("space", None, None),
        P("space", None),
        P("space", None, None, None),
    )
    out_specs = P(("ens", "space"), ("chan", "sub"))
    return jax.shard_map(
        on_any_device, mesh=mesh, in_specs=in_specs, out_specs=out_specs, check_vma=False
    )
```

```python
import math

import jax
import jax.numpy as jnp
from jax import lax
from jax.experimental import pallas as pl
from jax.experimental.pallas import tpu as pltpu
from jax.sharding import PartitionSpec as P

HD = 64


NORM_EPS = 1e-05
NEG_FILL = -1e30


def padded_2(array, sides, width):
    for axis, dim in sides:
        size, length = (lax.axis_size(axis), array.shape[dim])
        up = [(i, (i + 1) % size) for i in range(size - 1)]
        down = [(j, i) for i, j in up]
        last = lax.slice_in_dim(array, length - width, length, axis=dim)
        leading = lax.slice_in_dim(array, 0, width, axis=dim)
        before = lax.ppermute(last, axis, up)
        after = lax.ppermute(leading, axis, down)
        array = jnp.concatenate([before, array, after], axis=dim)
    return array


def normalize_rows(source, gain_row, shift_row):
    row_mean = jnp.mean(source, axis=-1, keepdims=True)
    spread = jnp.mean(source * source, axis=-1, keepdims=True) - row_mean * row_mean
    return (source - row_mean) * lax.rsqrt(spread + NORM_EPS) * gain_row + shift_row


def unpack_allowed(key_bits, key_ids, live_count, tile_size, blocks_own):
    shifts = jnp.arange(32, dtype=jnp.int32)
    expanded = jnp.right_shift(key_bits[..., None, :], shifts[:, None]) & 1
    lead_shape = key_bits.shape[:-2]
    expanded = expanded.reshape(lead_shape + (tile_size, tile_size))
    key_index = key_ids[..., None] * tile_size + jnp.arange(tile_size, dtype=jnp.int32)
    key_live = (key_ids[..., None] >= blocks_own) | (key_index < live_count)
    slot_count = key_ids.shape[-1]
    slot_first = jnp.arange(slot_count, dtype=jnp.int32)[:, None, None] == 0
    diagonal = (
        jnp.arange(tile_size, dtype=jnp.int32)[:, None]
        == jnp.arange(tile_size, dtype=jnp.int32)[None, :]
    )
    own_bit = slot_first & diagonal[None]
    return (expanded == 1) & (key_live[..., None] | own_bit)


def hidden_term(rows, in_piece, out_piece):
    hidden = jax.nn.gelu(
        lax.dot_general(
            rows, in_piece, (((1,), (1,)), ((), ())), preferred_element_type=jnp.float32
        )
    ).astype(jnp.bfloat16)
    return jnp.dot(hidden, out_piece, preferred_element_type=jnp.float32)


def on_device(
    node_state,
    norm_gains,
    norm_shifts,
    query_weight,
    key_weight,
    value_weight,
    out_weight,
    ffn_in,
    ffn_out,
    live_counts,
    send_rows,
    tile_keys,
    tile_bits,
):
    n_chan = lax.axis_size("chan")
    n_sub = lax.axis_size("sub")
    groups = n_chan * n_sub
    chan_at = lax.axis_index("chan")
    sub_at = lax.axis_index("sub")
    node_rank = chan_at * n_sub + sub_at
    node_count = node_state.shape[0]
    tile_size = tile_bits.shape[-1]
    word_count = tile_bits.shape[-2]
    slot_count = tile_keys.shape[1]
    blocks_own = tile_keys.shape[0]
    per_rank = node_count // groups
    head_cols = query_weight.shape[1]
    heads_here = head_cols // HD
    halo_rows = send_rows.shape[-1]
    live_count = live_counts[0]

    def own_half(source):
        step_rows = source.shape[0] // groups
        shaped = source.reshape((n_chan, n_sub, step_rows) + source.shape[1:])
        picked = lax.dynamic_index_in_dim(shaped, sub_at, 1, keepdims=False)
        return picked.reshape((n_chan * step_rows,) + source.shape[1:])

    node_rows = lax.all_to_all(node_state, ("chan", "sub"), split_axis=0, concat_axis=1, tiled=True)
    pair_weight = jnp.concatenate([key_weight, value_weight], axis=1)
    gathered = lax.all_gather(node_state, ("chan", "sub"), axis=1, tiled=True)
    normed = normalize_rows(gathered.astype(jnp.float32), norm_gains[0], norm_shifts[0]).astype(
        jnp.bfloat16
    )
    key_values = jnp.dot(normed, pair_weight, preferred_element_type=jnp.float32).astype(
        jnp.bfloat16
    )
    queries = jnp.dot(own_half(normed), query_weight, preferred_element_type=jnp.float32).astype(
        jnp.bfloat16
    )
    send_list = send_rows.reshape(2 * halo_rows)
    outgoing = jnp.take(key_values, send_list, axis=0)
    padded = padded_2(outgoing, (("space", 0),), halo_rows)
    extended = jnp.concatenate([key_values, padded[:halo_rows], padded[-halo_rows:]], axis=0)
    key_blocks = extended.reshape(-1, tile_size, 2 * head_cols)
    key_ids = own_half(tile_keys)
    key_bits = own_half(tile_bits)
    block_total = key_ids.shape[0]
    per_round = math.gcd(block_total, 4)
    rounds = block_total // per_round
    score_scale = 1.0 / math.sqrt(HD)

    def attend(inputs):
        q_part, id_part, bit_part = inputs
        chosen = key_blocks[id_part]
        keys_part = chosen[..., :head_cols].reshape(
            per_round, slot_count, tile_size, heads_here, HD
        )
        values_part = chosen[..., head_cols:].reshape(
            per_round, slot_count, tile_size, heads_here, HD
        )
        scores = (
            jnp.einsum("grhd,gtkhd->ghrtk", q_part, keys_part, preferred_element_type=jnp.float32)
            * score_scale
        )
        allowed = unpack_allowed(bit_part, id_part, live_count, tile_size, blocks_own)
        allowed = jnp.transpose(allowed, (0, 3, 1, 2))[:, None]
        masked = jnp.where(allowed, scores, NEG_FILL)
        row_max = jnp.max(masked, axis=(3, 4), keepdims=True)
        weights = jnp.where(allowed, jnp.exp(scores - row_max), 0.0)
        row_total = jnp.sum(weights, axis=(3, 4))
        mixed_heads = jnp.einsum(
            "ghrtk,gtkhd->grhd",
            weights.astype(jnp.bfloat16),
            values_part,
            preferred_element_type=jnp.float32,
        )
        mixed_heads = mixed_heads / jnp.transpose(row_total, (0, 2, 1))[..., None]
        return mixed_heads.astype(jnp.bfloat16).reshape(per_round * tile_size, head_cols)

    query_groups = queries.reshape(rounds, per_round, tile_size, heads_here, HD)
    attended = lax.map(
        attend,
        (
            query_groups,
            key_ids.reshape(rounds, per_round, slot_count),
            key_bits.reshape(rounds, per_round, slot_count, word_count, tile_size),
        ),
    )
    mixed_rows = jnp.dot(
        lax.all_to_all(
            attended.reshape(n_chan, per_rank, head_cols),
            "chan",
            split_axis=0,
            concat_axis=2,
            tiled=True,
        )[0],
        out_weight,
        preferred_element_type=jnp.float32,
    )
    after_attn = node_rows.astype(jnp.float32) + mixed_rows
    normed_two = normalize_rows(after_attn, norm_gains[1], norm_shifts[1]).astype(jnp.bfloat16)
    all_rows = lax.all_gather(normed_two, "chan", axis=0, tiled=True)
    update = lax.psum_scatter(
        hidden_term(all_rows, ffn_in, ffn_out).astype(jnp.bfloat16),
        "chan",
        scatter_dimension=0,
        tiled=True,
    ).astype(jnp.float32)
    position = node_rank * per_rank + jnp.arange(per_rank, dtype=jnp.int32)
    result = jnp.where((position < live_count)[:, None], after_attn + update, 0.0).astype(
        jnp.bfloat16
    )
    return lax.all_to_all(result, ("chan", "sub"), split_axis=1, concat_axis=0, tiled=True)


MESH = pl.DeviceIdType.MESH
LOG2E = 1.4426950408889634
NT = (((1,), (1,)), ((), ()))


def gelu_tanh(u):
    inner = 0.7978845608028654 * (u + 0.044715 * (u * u * u))
    return 0.5 * u * (1.0 + jnp.tanh(inner))


def layer_kernel(
    x_hbm,
    gains_hbm,
    shifts_hbm,
    wq_hbm,
    wk_hbm,
    wv_hbm,
    wo_hbm,
    fin_hbm,
    fout_hbm,
    live_hbm,
    send_hbm,
    tk_hbm,
    bits_hbm,
    out_ref,
    xq,
    gx,
    hsend,
    kv,
    wvt,
    qbuf,
    bias_ref,
    s_ref,
    o_ref,
    l_ref,
    att,
    full_part,
    half_part,
    from_sib,
    from_x,
    proj_w,
    ffn_w,
    norm_ref,
    send_ref,
    bits_ref,
    live_ref,
    tk_ref,
    w_sem,
    loc_sem,
    a_send,
    a_recv,
    x_send,
    x_recv,
    z_send,
    z_recv,
    h_send,
    h_recv,
    k_send,
    k_recv,
    t_send,
    t_recv,
    p_send,
    p_recv,
    d_send,
    d_recv,
):
    f32, bf16 = jnp.float32, jnp.bfloat16
    rows, cols = x_hbm.shape
    groups = gx.shape[0]
    tile = bits_hbm.shape[-1]
    words = bits_hbm.shape[-2]
    slots = tk_ref.shape[1]
    blocks_own = tk_ref.shape[0]
    halo = send_hbm.shape[-1]
    width, head_cols = wv_hbm.shape
    hidden_here = fin_hbm.shape[0]
    pw = 2 * HD
    pairs = head_cols // pw
    half = rows // 2
    n_here = half // tile
    n_halo = halo // tile
    n_keys = blocks_own + 2 * n_halo

    c = lax.axis_index("chan")
    s = lax.axis_index("sub")
    z = lax.axis_index("space")
    nz = lax.axis_size("space")
    own = c * 2 + s
    sib = c * 2 + 1 - s
    far = (1 - c) * 2
    xdev = {"chan": 1 - c}
    sdev = {"sub": 1 - s}
    has_up = z < nz - 1
    has_down = z > 0
    has_halo = jnp.where(s == 0, z, nz - 1 - z) > 0

    own_half = pl.ds(pl.multiple_of(s * half, half), half)
    sib_half = pl.ds(pl.multiple_of((1 - s) * half, half), half)
    local = pltpu.make_async_copy(x_hbm, xq, loc_sem.at[0])
    local_own = pltpu.make_async_copy(x_hbm.at[own_half], gx.at[own, pl.ds(0, half)], loc_sem.at[1])
    fin = ffn_w.at[pl.ds(0, hidden_here)]
    fout = ffn_w.at[pl.ds(hidden_here, hidden_here)]
    wo = ffn_w.at[pl.ds(2 * hidden_here, width)]
    n_norms = gains_hbm.shape[0]
    loads = (
        (send_hbm, send_ref, 0),
        (tk_hbm, tk_ref, 1),
        (live_hbm, live_ref, 2),
        (bits_hbm, bits_ref, 3),
        (wv_hbm, proj_w.at[:, pl.ds(2 * head_cols, head_cols)], 4),
        (gains_hbm, norm_ref.at[pl.ds(0, n_norms)], 5),
        (shifts_hbm, norm_ref.at[pl.ds(n_norms, n_norms)], 5),
        (wk_hbm, proj_w.at[:, pl.ds(0, head_cols)], 4),
        (wq_hbm, proj_w.at[:, pl.ds(head_cols, head_cols)], 4),
        (wo_hbm, wo, 6),
        (fin_hbm, fin, 6),
        (fout_hbm, fout, 6),
    )
    landed = (send_ref, tk_ref, live_ref, bits_ref, proj_w, norm_ref, ffn_w)

    def loaded(i):
        pltpu.make_async_copy(landed[i], landed[i], w_sem.at[i]).wait()


    barrier = pltpu.get_barrier_semaphore()

    def greet(dev):
        pl.semaphore_signal(barrier, inc=1, device_id=dev, device_id_type=MESH)

    greet(xdev)
    greet({"chan": 1 - c, "sub": 1 - s})
    greet(sdev)

    @pl.when(has_up)
    def _():
        greet({"space": z + 1})
        greet({"space": z + 1, "sub": 1 - s})

    @pl.when(has_down)
    def _():
        greet({"space": z - 1})
        greet({"space": z - 1, "sub": 1 - s})

    local.start()
    local_own.start()
    for a, b, i in loads:
        pltpu.make_async_copy(a, b, w_sem.at[i]).start()
    with jax.named_scope("barrierw"):
        pl.semaphore_wait(barrier, 3 + jnp.where(has_up, 2, 0) + jnp.where(has_down, 2, 0))
        local.wait()

    def rdma(src, dst, ss, rs, dev):
        return pltpu.make_async_remote_copy(
            src_ref=src, dst_ref=dst, send_sem=ss, recv_sem=rs, device_id=dev, device_id_type=MESH
        )

    def block(i):
        return pl.ds(pl.multiple_of(i * tile, tile), tile)

    def a_copy():
        return rdma(xq.at[sib_half], gx.at[own, pl.ds(0, half)], a_send, a_recv, sdev)

    def a_wait():
        part = gx.at[sib, pl.ds(0, half)]
        rdma(part, part, a_send, a_recv, sdev).wait_recv()

    def x_copy(i, to):
        src = xq.at[pl.ds(to * half + i * tile, tile)]
        dev = {"chan": 1 - c, "sub": to}
        return rdma(src, gx.at[own, block(i)], x_send, x_recv.at[i], dev)

    def x_wait(i):
        part = gx.at[pl.ds(far, 2), block(i)]
        rdma(part, part, x_send, x_recv.at[i], xdev).wait_recv()

    halo_at = pl.ds(half, halo)

    def z_copy(side):
        if side == 1:
            dev = {"space": z + 1, "sub": 0}
        else:
            dev = {"space": z - 1, "sub": 1}
        return rdma(hsend.at[side], gx.at[own, halo_at], z_send.at[side], z_recv, dev)

    def z_wait():
        part = gx.at[pl.ds(c * 2, 2), halo_at]
        rdma(part, part, z_send.at[0], z_recv, sdev).wait_recv()

    def h_copy(k):
        part = gx.at[pl.ds(c * 2, 2), pl.ds(half + k * tile, tile)]
        return rdma(part, part, h_send, h_recv.at[k], xdev)

    def h_wait(k):
        part = gx.at[pl.ds(far, 2), pl.ds(half + k * tile, tile)]
        rdma(part, part, h_send, h_recv.at[k], xdev).wait_recv()

    for i in range(n_here):
        x_copy(i, 0).start()
        x_copy(i, 1).start()
    a_copy().start()
    loaded(0)

    with jax.named_scope("onehot"):
        lanes = lax.broadcasted_iota(jnp.int32, (halo, tile), 1)
        for side in range(2):
            wanted = jnp.broadcast_to(send_ref[0, side : side + 1, :], (tile, halo)).T
            picks = jnp.concatenate(
                [(wanted == lanes + k * tile).astype(f32).astype(bf16) for k in range(rows // tile)],
                axis=1,
            )
            hsend[side] = jnp.dot(picks, xq[...], preferred_element_type=f32).astype(bf16)

    @pl.when(has_up)
    def _():
        z_copy(1).start()

    @pl.when(has_down)
    def _():
        z_copy(0).start()

    @pl.when(jnp.logical_not(has_halo))
    def _():
        gx[:, halo_at, :] = jnp.zeros((groups, halo, cols), bf16)

    for i in range(1, 5):
        loaded(i)
    wvt[...] = proj_w[:, 2 * head_cols :].astype(f32).T.astype(bf16)

    live = live_ref[0]
    word_rows = tile // words
    low_half = lax.broadcasted_iota(jnp.int32, (tile, pw), 1) < HD
    sub_row = lax.broadcasted_iota(jnp.int32, (8, tile), 0)
    phase = sub_row % 4
    high_nibble = sub_row // 4 * 4
    lane = lax.broadcasted_iota(jnp.int32, (words, tile), 1)
    first_key = lax.broadcasted_iota(jnp.int32, (words, tile), 0) * word_rows
    own_bit = jnp.where(
        lane // word_rows * word_rows == first_key,
        jnp.left_shift(jnp.ones_like(lane), lane % word_rows),
        0,
    )

    def mask_block(j, carry):
        b = s * n_here + j
        ids = [tk_ref[b, t] for t in range(slots)]
        spread = []
        for t in range(slots):
            limit = jnp.where(ids[t] >= blocks_own, tile, live - ids[t] * tile)
            count = jnp.clip(limit - first_key, 0, word_rows)
            some = jnp.left_shift(jnp.ones_like(count), jnp.minimum(count, word_rows - 1)) - 1
            good = jnp.where(count >= word_rows, -1, some)
            if t == 0:
                good = good | own_bit
            kept = bits_ref[b, t] & good
            spread.append(
                [
                    jnp.right_shift(jnp.broadcast_to(kept[w : w + 1, :], (8, tile)), phase)
                    & 0x11111111
                    for w in range(words)
                ]
            )
        for e in range(n_keys):
            picks = [jnp.where(ids[t] == e, -1, 0) for t in range(slots)]
            for w in range(words):
                total = spread[0][w] & picks[0]
                for t in range(1, slots):
                    total = total + (spread[t][w] & picks[t])
                for m in range(word_rows // 8):
                    times = jnp.right_shift(total, high_nibble + 8 * m) & 15
                    at = e * tile + w * word_rows + m * 8
                    bias_ref[j, at : at + 8] = jnp.maximum(jnp.log2(times.astype(f32)), NEG_FILL)
        return carry

    with jax.named_scope("mask"):
        lax.fori_loop(0, n_here, mask_block, 0)

    def full_rows(at):
        return jnp.concatenate([gx[g, at] for g in range(groups)], axis=1).astype(f32)

    def norm(v, which):
        mean = jnp.mean(v, axis=-1, keepdims=True)
        spread = jnp.mean(v * v, axis=-1, keepdims=True) - mean * mean
        scaled = (v - mean) * lax.rsqrt(spread + NORM_EPS)
        gain, shift = norm_ref[which : which + 1, :], norm_ref[n_norms + which : n_norms + which + 1, :]
        return scaled * gain + shift

    scale = LOG2E / math.sqrt(HD)

    per_core = n_here + n_halo

    def k_copy(core, i):
        part = kv.at[core * per_core + i]
        return rdma(part, part, k_send.at[0], k_recv.at[i], sdev)

    def project(i, with_queries):
        normed = norm(full_rows(block(i)), 0).astype(bf16)
        to = s * per_core + i
        wanted = (2 if with_queries else 1) * head_cols
        both = jnp.dot(normed, proj_w[:, :wanted], preferred_element_type=f32)
        for pair in range(pairs):
            kv[to, pair] = both[:, pair * pw : (pair + 1) * pw].astype(bf16)
        if with_queries:
            qbuf[block(i)] = (both[:, head_cols:] * scale).astype(bf16)
        values = lax.dot_general(wvt[...], normed, NT, preferred_element_type=f32)
        for pair in range(pairs):
            kv[to, pairs + pair] = values[pair * pw : (pair + 1) * pw].astype(bf16)
        k_copy(s, i).start()

    loaded(5)
    local_own.wait()
    with jax.named_scope("aw"):
        a_wait()

    def own_step(i, carry):
        with jax.named_scope("xw"):
            x_wait(i)
        with jax.named_scope("proj"):
            project(i, True)
        return carry

    early = n_here // 2
    lax.fori_loop(0, early, own_step, 0)

    with jax.named_scope("zw"):

        @pl.when(has_halo)
        def _():
            z_wait()
            for k in range(n_halo):
                h_copy(k).start()

    lax.fori_loop(early, n_here, own_step, 0)
    def t_copy(j):
        part = att.at[pl.ds(c * pairs, pairs), block(j)]
        return rdma(part, part, t_send, t_recv.at[j], xdev)

    def t_wait(j):
        part = att.at[pl.ds((1 - c) * pairs, pairs), block(j)]
        rdma(part, part, t_send, t_recv.at[j], xdev).wait_recv()

    def stored(e):
        if e < blocks_own:
            return e // n_here * per_core + e % n_here
        e -= blocks_own
        return e // n_halo * per_core + n_here + e % n_halo

    ones = jnp.ones((16, 2 * tile), bf16)

    def scores_of(j, pair, keys_at):
        q_pair = qbuf[block(j), pair * pw : (pair + 1) * pw]
        zero = jnp.zeros_like(q_pair)
        wide = jnp.concatenate(
            [jnp.where(low_half, q_pair, zero), jnp.where(low_half, zero, q_pair)], axis=0
        )
        top = jnp.full((8, 2 * tile), NEG_FILL, f32)
        for n, e in enumerate(keys_at):
            bias = bias_ref[j, e * tile : (e + 1) * tile]
            scores = lax.dot_general(kv[stored(e), pair], wide, NT, preferred_element_type=f32)
            scores = scores + jnp.concatenate([bias, bias], axis=1)
            s_ref[pair, n * tile : (n + 1) * tile] = scores
            top = jnp.maximum(top, jnp.max(scores.reshape(tile // 8, 8, 2 * tile), axis=0))
        return jnp.max(top, axis=0, keepdims=True)

    def mixed_of(pair, keys_at, top):
        mixed = jnp.zeros((pw + 16, 2 * tile), f32)
        for n in range(0, len(keys_at), 2):
            p = jnp.exp2(s_ref[pair, n * tile : (n + 2) * tile] - top).astype(bf16)
            values = jnp.concatenate(
                [kv[stored(keys_at[n]), pairs + pair], kv[stored(keys_at[n + 1]), pairs + pair]],
                axis=1,
            )
            values = jnp.concatenate([values, ones], axis=0)
            mixed = mixed + jnp.dot(values, p, preferred_element_type=f32)
        heads = jnp.concatenate([mixed[:HD, :tile], mixed[HD:pw, tile:]], axis=0)
        return heads, mixed[pw : pw + 8]

    def both_heads(row):
        return jnp.concatenate(
            [
                jnp.broadcast_to(row[:, :tile], (HD, tile)),
                jnp.broadcast_to(row[:, tile:], (HD, tile)),
            ],
            axis=0,
        )

    own_keys = tuple(range(blocks_own))
    halo_keys = tuple(range(blocks_own, n_keys))

    def attend_own(j):
        tops = [scores_of(j, pair, own_keys) for pair in range(pairs)]
        for pair in range(pairs):
            heads, sums = mixed_of(pair, own_keys, tops[pair])
            o_ref[j, pair] = heads
            l_ref[j, pair, :8] = sums
            l_ref[j, pair, 8:] = jnp.broadcast_to(tops[pair], (8, 2 * tile))

    def attend_halo(j):
        tops = [scores_of(j, pair, halo_keys) for pair in range(pairs)]
        for pair in range(pairs):
            before = l_ref[j, pair, 8:9]
            top = jnp.maximum(tops[pair], before)
            shrink = jnp.exp2(before - top)
            heads, sums = mixed_of(pair, halo_keys, top)
            total = l_ref[j, pair, :1] * shrink + sums[:1]
            heads = o_ref[j, pair] * both_heads(shrink) + heads
            heads = heads * both_heads(1.0 / total)
            att[c * pairs + pair, block(j)] = heads.T.astype(bf16)
        t_copy(j).start()

    with jax.named_scope("kvw"):
        for i in range(n_here):
            k_copy(1 - s, i).wait_recv()

    def halo_step(k, carry):
        with jax.named_scope("hw"):

            @pl.when(has_halo)
            def _():
                h_wait(k)

        with jax.named_scope("hproj"):
            project(n_here + k, False)
        return carry

    def first_step(j, carry):
        with jax.named_scope("aown"):
            attend_own(j)
        return carry

    lax.fori_loop(0, 1, first_step, 0)
    lax.fori_loop(0, n_halo, halo_step, 0)
    lax.fori_loop(1, early, first_step, 0)
    with jax.named_scope("kvw2"):
        for i in range(n_here, n_here + n_halo):
            k_copy(1 - s, i).wait_recv()

    def second_step(j, carry):
        with jax.named_scope("ahalo"):
            attend_halo(j)
        with jax.named_scope("aown"):
            attend_own(j + early)
        return carry

    def third_step(j, carry):
        with jax.named_scope("ahalo"):
            attend_halo(j)
        return carry

    lax.fori_loop(0, n_here - early, second_step, 0)
    lax.fori_loop(n_here - early, n_here, third_step, 0)

    loaded(6)

    def p_copy(j, to):
        src = half_part.at[j, far + to]
        dev = {"chan": 1 - c, "sub": to}
        return rdma(src, from_x.at[j, s], p_send, p_recv.at[j], dev)

    def p_wait(j):
        part = from_x.at[j]
        rdma(part, part, p_send, p_recv.at[j], xdev).wait_recv()

    def d_copy(j):
        return rdma(full_part.at[j, sib], from_sib.at[j], d_send, d_recv.at[j], sdev)

    def ffn_block(j, carry):
        with jax.named_scope("tw"):
            t_wait(j)
        at = block(j)
        mixed = jnp.concatenate([att[g, at] for g in range(2 * pairs)], axis=1)
        after = full_rows(at) + jnp.dot(mixed, wo[...], preferred_element_type=f32)
        normed_two = norm(after, 1).astype(bf16)
        hidden = gelu_tanh(
            lax.dot_general(normed_two, fin[...], NT, preferred_element_type=f32)
        ).astype(bf16)
        part = jnp.dot(hidden, fout[...], preferred_element_type=f32)
        for g in range(groups):
            half_part[j, g] = part[:, g * cols : (g + 1) * cols].astype(bf16)
        p_copy(j, 0).start()
        p_copy(j, 1).start()
        whole = part + after
        for g in range(groups):
            full_part[j, g] = whole[:, g * cols : (g + 1) * cols]
        d_copy(j).start()
        return carry

    with jax.named_scope("ffn"):
        lax.fori_loop(0, n_here, ffn_block, 0)

    in_block = lax.broadcasted_iota(jnp.int32, (tile, cols), 0)

    def finish(j, carry):
        with jax.named_scope("pw"):
            d_copy(j).wait_recv()
            p_wait(j)
        for core, kept in ((s, full_part[j, own]), (1 - s, from_sib[j])):
            base = core * half + j * tile
            summed = kept + from_x[j, core].astype(f32)
            done = jnp.where(base + in_block < live, summed, 0.0).astype(bf16)
            out_ref[pl.ds(pl.multiple_of(base, tile), tile)] = done
        return carry

    with jax.named_scope("finish"):
        lax.fori_loop(0, n_here, finish, 0)

    def sent(part, sem):
        rdma(part, part, sem, sem, sdev).wait_send()

    with jax.named_scope("endw"):
        sent(xq, x_send)
        sent(xq.at[own_half], a_send)
        sent(kv.at[pl.ds(s * per_core, per_core)], k_send.at[0])
        sent(att.at[pl.ds(c * pairs, pairs)], t_send)
        sent(half_part.at[:, pl.ds(far, 2)], p_send)
        sent(from_sib, d_send)

        @pl.when(has_up)
        def _():
            z_copy(1).wait_send()

        @pl.when(has_down)
        def _():
            z_copy(0).wait_send()

        @pl.when(has_halo)
        def _():
            sent(gx.at[pl.ds(c * 2, 2), halo_at], h_send)


def one_kernel(*args):
    (x, gains, shifts, wq, wk, wv, wo, fin, fout, live, send, tk, bits) = args
    f32, bf16 = jnp.float32, jnp.bfloat16
    rows, cols = x.shape
    width = gains.shape[1]
    groups = lax.axis_size("chan") * lax.axis_size("sub")
    halo = send.shape[-1]
    tile = bits.shape[-1]
    slots = tk.shape[1]
    ext = rows + 2 * halo
    head_cols = wq.shape[1]
    half = rows // 2
    pairs = head_cols // (2 * HD)
    n_here = half // tile
    n_halo = halo // tile
    vmem = pltpu.VMEM
    dma = pltpu.SemaphoreType.DMA
    in_any = pl.BlockSpec(memory_space=pl.ANY)
    return pl.pallas_call(
        layer_kernel,
        out_shape=pltpu.VMEM(x.shape, bf16),
        in_specs=[in_any] * 13,
        out_specs=pl.BlockSpec(memory_space=pltpu.VMEM),
        scratch_shapes=[
            vmem(x.shape, bf16),
            vmem((groups, half + halo, cols), bf16),
            vmem((2, halo, cols), bf16),
            vmem((ext // tile, 2 * pairs, tile, 2 * HD), bf16),
            vmem((head_cols, width), bf16),
            vmem((half, head_cols), bf16),
            vmem((n_here, ext, tile), f32),
            vmem((pairs, rows, 2 * tile), f32),
            vmem((n_here, pairs, 2 * HD, tile), f32),
            vmem((n_here, pairs, 16, 2 * tile), f32),
            vmem((2 * pairs, half, 2 * HD), bf16),
            vmem((n_here, groups, tile, cols), f32),
            vmem((n_here, groups, tile, cols), bf16),
            vmem((n_here, tile, cols), f32),
            vmem((n_here, 2, tile, cols), bf16),
            vmem((width, 3 * head_cols), bf16),
            vmem((2 * fin.shape[0] + wo.shape[0], width), bf16),
            vmem((2 * gains.shape[0], width), f32),
            vmem(send.shape, jnp.int32),
            vmem(bits.shape, jnp.int32),
            pltpu.SMEM(live.shape, jnp.int32),
            pltpu.SMEM(tk.shape, jnp.int32),
            dma((7,)),
            dma((2,)),
            dma,
            dma,
            dma,
            dma((n_here,)),
            dma((2,)),
            dma,
            dma,
            dma((n_halo,)),
            dma((1,)),
            dma((n_here + n_halo,)),
            dma,
            dma((n_here,)),
            dma,
            dma((n_here,)),
            dma,
            dma((n_here,)),
        ],
        compiler_params=pltpu.CompilerParams(collective_id=0, has_side_effects=True),
    )(*args)


def on_any_device(*args):
    two_by_two = lax.axis_size("chan") == 2 and lax.axis_size("sub") == 2
    cols, head_cols = args[0].shape[1], args[3].shape[1]
    tile, halo = args[12].shape[-1], args[10].shape[-1]
    rows_fit = args[0].shape[0] % (4 * tile) == 0 and halo % (2 * tile) == 0
    few_slots = args[11].shape[1] < 16 and args[12].shape[-2] * 32 == tile and tile == cols
    if two_by_two and cols % 128 == 0 and head_cols % (2 * HD) == 0 and rows_fit and few_slots:
        return one_kernel(*args)
    return on_device(*args)


def solution(mesh):
    in_specs = (
        P(("ens", "space"), ("chan", "sub")),
        P(),
        P(),
        P(None, "chan"),
        P(None, "chan"),
        P(None, "chan"),
        P(),
        P("chan", None),
        P("chan", None),
        P("space"),
        P("space", None, None),
        P("space", None),
        P("space", None, None, None),
    )
    out_specs = P(("ens", "space"), ("chan", "sub"))
    return jax.shard_map(
        on_any_device, mesh=mesh, in_specs=in_specs, out_specs=out_specs, check_vma=False
    )
```

```python
import math

import jax
import jax.numpy as jnp
from jax import lax
from jax.experimental import pallas as pl
from jax.experimental.pallas import tpu as pltpu
from jax.sharding import PartitionSpec as P

HD = 64


NORM_EPS = 1e-05
NEG_FILL = -1e30


def padded_2(array, sides, width):
    for axis, dim in sides:
        size, length = (lax.axis_size(axis), array.shape[dim])
        up = [(i, (i + 1) % size) for i in range(size - 1)]
        down = [(j, i) for i, j in up]
        last = lax.slice_in_dim(array, length - width, length, axis=dim)
        leading = lax.slice_in_dim(array, 0, width, axis=dim)
        before = lax.ppermute(last, axis, up)
        after = lax.ppermute(leading, axis, down)
        array = jnp.concatenate([before, array, after], axis=dim)
    return array


def normalize_rows(source, gain_row, shift_row):
    row_mean = jnp.mean(source, axis=-1, keepdims=True)
    spread = jnp.mean(source * source, axis=-1, keepdims=True) - row_mean * row_mean
    return (source - row_mean) * lax.rsqrt(spread + NORM_EPS) * gain_row + shift_row


def unpack_allowed(key_bits, key_ids, live_count, tile_size, blocks_own):
    shifts = jnp.arange(32, dtype=jnp.int32)
    expanded = jnp.right_shift(key_bits[..., None, :], shifts[:, None]) & 1
    lead_shape = key_bits.shape[:-2]
    expanded = expanded.reshape(lead_shape + (tile_size, tile_size))
    key_index = key_ids[..., None] * tile_size + jnp.arange(tile_size, dtype=jnp.int32)
    key_live = (key_ids[..., None] >= blocks_own) | (key_index < live_count)
    slot_count = key_ids.shape[-1]
    slot_first = jnp.arange(slot_count, dtype=jnp.int32)[:, None, None] == 0
    diagonal = (
        jnp.arange(tile_size, dtype=jnp.int32)[:, None]
        == jnp.arange(tile_size, dtype=jnp.int32)[None, :]
    )
    own_bit = slot_first & diagonal[None]
    return (expanded == 1) & (key_live[..., None] | own_bit)


def hidden_term(rows, in_piece, out_piece):
    hidden = jax.nn.gelu(
        lax.dot_general(
            rows, in_piece, (((1,), (1,)), ((), ())), preferred_element_type=jnp.float32
        )
    ).astype(jnp.bfloat16)
    return jnp.dot(hidden, out_piece, preferred_element_type=jnp.float32)


def on_device(
    node_state,
    norm_gains,
    norm_shifts,
    query_weight,
    key_weight,
    value_weight,
    out_weight,
    ffn_in,
    ffn_out,
    live_counts,
    send_rows,
    tile_keys,
    tile_bits,
):
    n_chan = lax.axis_size("chan")
    n_sub = lax.axis_size("sub")
    groups = n_chan * n_sub
    chan_at = lax.axis_index("chan")
    sub_at = lax.axis_index("sub")
    node_rank = chan_at * n_sub + sub_at
    node_count = node_state.shape[0]
    tile_size = tile_bits.shape[-1]
    word_count = tile_bits.shape[-2]
    slot_count = tile_keys.shape[1]
    blocks_own = tile_keys.shape[0]
    per_rank = node_count // groups
    head_cols = query_weight.shape[1]
    heads_here = head_cols // HD
    halo_rows = send_rows.shape[-1]
    live_count = live_counts[0]

    def own_half(source):
        step_rows = source.shape[0] // groups
        shaped = source.reshape((n_chan, n_sub, step_rows) + source.shape[1:])
        picked = lax.dynamic_index_in_dim(shaped, sub_at, 1, keepdims=False)
        return picked.reshape((n_chan * step_rows,) + source.shape[1:])

    node_rows = lax.all_to_all(node_state, ("chan", "sub"), split_axis=0, concat_axis=1, tiled=True)
    pair_weight = jnp.concatenate([key_weight, value_weight], axis=1)
    gathered = lax.all_gather(node_state, ("chan", "sub"), axis=1, tiled=True)
    normed = normalize_rows(gathered.astype(jnp.float32), norm_gains[0], norm_shifts[0]).astype(
        jnp.bfloat16
    )
    key_values = jnp.dot(normed, pair_weight, preferred_element_type=jnp.float32).astype(
        jnp.bfloat16
    )
    queries = jnp.dot(own_half(normed), query_weight, preferred_element_type=jnp.float32).astype(
        jnp.bfloat16
    )
    send_list = send_rows.reshape(2 * halo_rows)
    outgoing = jnp.take(key_values, send_list, axis=0)
    padded = padded_2(outgoing, (("space", 0),), halo_rows)
    extended = jnp.concatenate([key_values, padded[:halo_rows], padded[-halo_rows:]], axis=0)
    key_blocks = extended.reshape(-1, tile_size, 2 * head_cols)
    key_ids = own_half(tile_keys)
    key_bits = own_half(tile_bits)
    block_total = key_ids.shape[0]
    per_round = math.gcd(block_total, 4)
    rounds = block_total // per_round
    score_scale = 1.0 / math.sqrt(HD)

    def attend(inputs):
        q_part, id_part, bit_part = inputs
        chosen = key_blocks[id_part]
        keys_part = chosen[..., :head_cols].reshape(
            per_round, slot_count, tile_size, heads_here, HD
        )
        values_part = chosen[..., head_cols:].reshape(
            per_round, slot_count, tile_size, heads_here, HD
        )
        scores = (
            jnp.einsum("grhd,gtkhd->ghrtk", q_part, keys_part, preferred_element_type=jnp.float32)
            * score_scale
        )
        allowed = unpack_allowed(bit_part, id_part, live_count, tile_size, blocks_own)
        allowed = jnp.transpose(allowed, (0, 3, 1, 2))[:, None]
        masked = jnp.where(allowed, scores, NEG_FILL)
        row_max = jnp.max(masked, axis=(3, 4), keepdims=True)
        weights = jnp.where(allowed, jnp.exp(scores - row_max), 0.0)
        row_total = jnp.sum(weights, axis=(3, 4))
        mixed_heads = jnp.einsum(
            "ghrtk,gtkhd->grhd",
            weights.astype(jnp.bfloat16),
            values_part,
            preferred_element_type=jnp.float32,
        )
        mixed_heads = mixed_heads / jnp.transpose(row_total, (0, 2, 1))[..., None]
        return mixed_heads.astype(jnp.bfloat16).reshape(per_round * tile_size, head_cols)

    query_groups = queries.reshape(rounds, per_round, tile_size, heads_here, HD)
    attended = lax.map(
        attend,
        (
            query_groups,
            key_ids.reshape(rounds, per_round, slot_count),
            key_bits.reshape(rounds, per_round, slot_count, word_count, tile_size),
        ),
    )
    mixed_rows = jnp.dot(
        lax.all_to_all(
            attended.reshape(n_chan, per_rank, head_cols),
            "chan",
            split_axis=0,
            concat_axis=2,
            tiled=True,
        )[0],
        out_weight,
        preferred_element_type=jnp.float32,
    )
    after_attn = node_rows.astype(jnp.float32) + mixed_rows
    normed_two = normalize_rows(after_attn, norm_gains[1], norm_shifts[1]).astype(jnp.bfloat16)
    all_rows = lax.all_gather(normed_two, "chan", axis=0, tiled=True)
    update = lax.psum_scatter(
        hidden_term(all_rows, ffn_in, ffn_out).astype(jnp.bfloat16),
        "chan",
        scatter_dimension=0,
        tiled=True,
    ).astype(jnp.float32)
    position = node_rank * per_rank + jnp.arange(per_rank, dtype=jnp.int32)
    result = jnp.where((position < live_count)[:, None], after_attn + update, 0.0).astype(
        jnp.bfloat16
    )
    return lax.all_to_all(result, ("chan", "sub"), split_axis=1, concat_axis=0, tiled=True)


MESH = pl.DeviceIdType.MESH
LOG2E = 1.4426950408889634
NT = (((1,), (1,)), ((), ()))


def gelu_tanh(u):
    inner = 0.7978845608028654 * (u + 0.044715 * (u * u * u))
    return 0.5 * u * (1.0 + jnp.tanh(inner))


def layer_kernel(
    x_hbm,
    gains_hbm,
    shifts_hbm,
    wq_hbm,
    wk_hbm,
    wv_hbm,
    wo_hbm,
    fin_hbm,
    fout_hbm,
    live_hbm,
    send_hbm,
    tk_hbm,
    bits_hbm,
    out_ref,
    xq,
    gx,
    hsend,
    kv,
    wvt,
    qbuf,
    bias_ref,
    s_ref,
    o_ref,
    l_ref,
    att,
    full_part,
    half_part,
    from_sib,
    from_x,
    proj_w,
    ffn_w,
    norm_ref,
    send_ref,
    bits_ref,
    live_ref,
    tk_ref,
    w_sem,
    loc_sem,
    a_send,
    a_recv,
    x_send,
    x_recv,
    z_send,
    z_recv,
    h_send,
    h_recv,
    k_send,
    k_recv,
    t_send,
    t_recv,
    p_send,
    d_send,
    d_recv,
):
    f32, bf16 = jnp.float32, jnp.bfloat16
    rows, cols = x_hbm.shape
    groups = gx.shape[0]
    tile = bits_hbm.shape[-1]
    words = bits_hbm.shape[-2]
    slots = tk_ref.shape[1]
    blocks_own = tk_ref.shape[0]
    halo = send_hbm.shape[-1]
    width, head_cols = wv_hbm.shape
    hidden_here = fin_hbm.shape[0]
    pw = 2 * HD
    pairs = head_cols // pw
    half = rows // 2
    n_here = half // tile
    n_halo = halo // tile
    n_keys = blocks_own + 2 * n_halo

    c = lax.axis_index("chan")
    s = lax.axis_index("sub")
    z = lax.axis_index("space")
    nz = lax.axis_size("space")
    own = c * 2 + s
    sib = c * 2 + 1 - s
    far = (1 - c) * 2
    xdev = {"chan": 1 - c}
    sdev = {"sub": 1 - s}
    has_up = z < nz - 1
    has_down = z > 0
    has_halo = jnp.where(s == 0, z, nz - 1 - z) > 0
    sib_halo = jnp.where(s == 0, nz - 1 - z, z) > 0
    per_core = n_here + n_halo
    last = n_here - 1

    own_half = pl.ds(pl.multiple_of(s * half, half), half)
    sib_half = pl.ds(pl.multiple_of((1 - s) * half, half), half)
    local = pltpu.make_async_copy(x_hbm, xq, loc_sem.at[0])
    local_own = pltpu.make_async_copy(x_hbm.at[own_half], gx.at[own, pl.ds(0, half)], loc_sem.at[1])
    fin = ffn_w.at[pl.ds(0, hidden_here)]
    fout = ffn_w.at[pl.ds(hidden_here, hidden_here)]
    wo = ffn_w.at[pl.ds(2 * hidden_here, width)]
    n_norms = gains_hbm.shape[0]
    loads = (
        (send_hbm, send_ref, 0),
        (tk_hbm, tk_ref, 1),
        (live_hbm, live_ref, 2),
        (bits_hbm, bits_ref, 3),
        (wv_hbm, proj_w.at[:, pl.ds(2 * head_cols, head_cols)], 4),
        (gains_hbm, norm_ref.at[pl.ds(0, n_norms)], 5),
        (shifts_hbm, norm_ref.at[pl.ds(n_norms, n_norms)], 5),
        (wk_hbm, proj_w.at[:, pl.ds(0, head_cols)], 4),
        (wq_hbm, proj_w.at[:, pl.ds(head_cols, head_cols)], 4),
        (wo_hbm, wo, 6),
        (fin_hbm, fin, 6),
        (fout_hbm, fout, 6),
    )
    landed = (send_ref, tk_ref, live_ref, bits_ref, proj_w, norm_ref, ffn_w)

    def loaded(i):
        pltpu.make_async_copy(landed[i], landed[i], w_sem.at[i]).wait()


    barrier = pltpu.get_barrier_semaphore()

    def greet(dev):
        pl.semaphore_signal(barrier, inc=1, device_id=dev, device_id_type=MESH)

    greet(xdev)
    greet({"chan": 1 - c, "sub": 1 - s})
    greet(sdev)

    @pl.when(has_up)
    def _():
        greet({"space": z + 1})
        greet({"space": z + 1, "sub": 1 - s})

    @pl.when(has_down)
    def _():
        greet({"space": z - 1})
        greet({"space": z - 1, "sub": 1 - s})

    local.start()
    local_own.start()
    for a, b, i in loads:
        pltpu.make_async_copy(a, b, w_sem.at[i]).start()
    with jax.named_scope("barrierw"):
        pl.semaphore_wait(barrier, 3 + jnp.where(has_up, 2, 0) + jnp.where(has_down, 2, 0))
    with jax.named_scope("localw"):
        local.wait()

    def rdma(src, dst, ss, rs, dev):
        return pltpu.make_async_remote_copy(
            src_ref=src, dst_ref=dst, send_sem=ss, recv_sem=rs, device_id=dev, device_id_type=MESH
        )

    def block(i):
        return pl.ds(pl.multiple_of(i * tile, tile), tile)

    def a_copy():
        return rdma(xq.at[sib_half], gx.at[own, pl.ds(0, half)], a_send, a_recv, sdev)

    def a_wait():
        part = gx.at[sib, pl.ds(0, half)]
        rdma(part, part, a_send, a_recv, sdev).wait_recv()

    def x_copy(i, to):
        src = xq.at[pl.ds(to * half + i * tile, tile)]
        dev = {"chan": 1 - c, "sub": to}
        return rdma(src, gx.at[own, block(i)], x_send, x_recv.at[i], dev)

    def x_wait(i):
        part = gx.at[pl.ds(far, 2), block(i)]
        rdma(part, part, x_send, x_recv.at[i], xdev).wait_recv()

    halo_at = pl.ds(half, halo)

    def z_copy(side):
        if side == 1:
            dev = {"space": z + 1, "sub": 0}
        else:
            dev = {"space": z - 1, "sub": 1}
        return rdma(hsend.at[side], gx.at[own, halo_at], z_send.at[side], z_recv, dev)

    def z_wait():
        part = gx.at[pl.ds(c * 2, 2), halo_at]
        rdma(part, part, z_send.at[0], z_recv, sdev).wait_recv()

    def h_copy(k):
        part = gx.at[pl.ds(c * 2, 2), pl.ds(half + k * tile, tile)]
        return rdma(part, part, h_send, h_recv.at[k], xdev)

    def h_wait(k):
        part = gx.at[pl.ds(far, 2), pl.ds(half + k * tile, tile)]
        rdma(part, part, h_send, h_recv.at[k], xdev).wait_recv()

    for i in range(last):
        x_copy(i, 0).start()
        x_copy(i, 1).start()
    a_copy().start()
    loaded(0)

    with jax.named_scope("onehot"):
        lanes = lax.broadcasted_iota(jnp.int32, (halo, tile), 1)
        for side in range(2):
            wanted = jnp.broadcast_to(send_ref[0, side : side + 1, :], (tile, halo)).T
            picks = jnp.concatenate(
                [(wanted == lanes + k * tile).astype(f32).astype(bf16) for k in range(rows // tile)],
                axis=1,
            )
            hsend[side] = jnp.dot(picks, xq[...], preferred_element_type=f32).astype(bf16)

    @pl.when(has_up)
    def _():
        z_copy(1).start()

    @pl.when(has_down)
    def _():
        z_copy(0).start()

    for core, there in ((s, has_halo), (1 - s, sib_halo)):

        @pl.when(jnp.logical_not(there))
        def _():
            empty = jnp.zeros((n_halo, 2 * pairs, tile, pw), bf16)
            kv[pl.ds(core * per_core + n_here, n_halo)] = empty

    for i in range(1, 5):
        loaded(i)
    wvt[...] = proj_w[:, 2 * head_cols :].astype(f32).T.astype(bf16)

    live = live_ref[0]
    word_rows = tile // words
    low_half = lax.broadcasted_iota(jnp.int32, (tile, pw), 1) < HD
    sub_row = lax.broadcasted_iota(jnp.int32, (8, tile), 0)
    phase = sub_row % 4
    high_nibble = sub_row // 4 * 4
    lane = lax.broadcasted_iota(jnp.int32, (words, tile), 1)
    first_key = lax.broadcasted_iota(jnp.int32, (words, tile), 0) * word_rows
    own_bit = jnp.where(
        lane // word_rows * word_rows == first_key,
        jnp.left_shift(jnp.ones_like(lane), lane % word_rows),
        0,
    )

    def mask_block(j, carry):
        b = s * n_here + j
        ids = [tk_ref[b, t] for t in range(slots)]
        spread = []
        for t in range(slots):
            limit = jnp.where(ids[t] >= blocks_own, tile, live - ids[t] * tile)
            count = jnp.clip(limit - first_key, 0, word_rows)
            some = jnp.left_shift(jnp.ones_like(count), jnp.minimum(count, word_rows - 1)) - 1
            good = jnp.where(count >= word_rows, -1, some)
            if t == 0:
                good = good | own_bit
            kept = bits_ref[b, t] & good
            spread.append(
                [
                    jnp.right_shift(jnp.broadcast_to(kept[w : w + 1, :], (8, tile)), phase)
                    & 0x11111111
                    for w in range(words)
                ]
            )
        for e in range(n_keys):
            picks = [jnp.where(ids[t] == e, -1, 0) for t in range(slots)]
            for w in range(words):
                total = spread[0][w] & picks[0]
                for t in range(1, slots):
                    total = total + (spread[t][w] & picks[t])
                for m in range(word_rows // 8):
                    times = jnp.right_shift(total, high_nibble + 8 * m) & 15
                    at = e * tile + w * word_rows + m * 8
                    bias_ref[j, at : at + 8] = jnp.maximum(jnp.log2(times.astype(f32)), NEG_FILL)
        return carry

    with jax.named_scope("mask"):
        lax.fori_loop(0, n_here, mask_block, 0)

    def full_rows(at):
        return jnp.concatenate([gx[g, at] for g in range(groups)], axis=1).astype(f32)

    def norm(v, which):
        mean = jnp.mean(v, axis=-1, keepdims=True)
        spread = jnp.mean(v * v, axis=-1, keepdims=True) - mean * mean
        scaled = (v - mean) * lax.rsqrt(spread + NORM_EPS)
        gain, shift = norm_ref[which : which + 1, :], norm_ref[n_norms + which : n_norms + which + 1, :]
        return scaled * gain + shift

    scale = LOG2E / math.sqrt(HD)

    def k_copy(i, kind):
        part = kv.at[s * per_core + i]
        return rdma(part, part, k_send.at[kind % 2], k_recv.at[kind], sdev)

    def k_wait(first, count, kind):
        part = kv.at[pl.ds((1 - s) * per_core + first, count)]
        rdma(part, part, k_send.at[0], k_recv.at[kind], sdev).wait_recv()

    def project(i, kind):
        with_queries = kind != 1
        normed = norm(full_rows(block(i)), 0).astype(bf16)
        to = s * per_core + i
        wanted = (2 if with_queries else 1) * head_cols
        both = jnp.dot(normed, proj_w[:, :wanted], preferred_element_type=f32)
        for pair in range(pairs):
            kv[to, pair] = both[:, pair * pw : (pair + 1) * pw].astype(bf16)
        if with_queries:
            qbuf[block(i)] = (both[:, head_cols:] * scale).astype(bf16)
        values = lax.dot_general(wvt[...], normed, NT, preferred_element_type=f32)
        for pair in range(pairs):
            kv[to, pairs + pair] = values[pair * pw : (pair + 1) * pw].astype(bf16)
        k_copy(i, kind).start()

    loaded(5)
    local_own.wait()
    with jax.named_scope("aw"):
        a_wait()

    def own_step(i, carry):
        with jax.named_scope("xw"):
            x_wait(i)
        with jax.named_scope("proj"):
            project(i, 0)
        return carry

    lax.fori_loop(0, 1, own_step, 0)

    with jax.named_scope("zw"):

        @pl.when(has_halo)
        def _():
            z_wait()
            for k in range(n_halo):
                h_copy(k).start()

    x_copy(last, 0).start()
    x_copy(last, 1).start()
    lax.fori_loop(1, last, own_step, 0)

    @pl.when(has_halo)
    def _():
        def halo_step(k, carry):
            with jax.named_scope("hw"):
                h_wait(k)
            with jax.named_scope("hproj"):
                project(n_here + k, 1)
            return carry

        lax.fori_loop(0, n_halo, halo_step, 0)

    with jax.named_scope("xw"):
        x_wait(last)
    with jax.named_scope("proj"):
        project(last, 2)

    def t_copy(j, first, count):
        part = att.at[pl.ds(c * pairs + first, count), block(j)]
        return rdma(part, part, t_send, t_recv.at[j], xdev)

    def t_wait(j):
        part = att.at[pl.ds((1 - c) * pairs, pairs), block(j)]
        rdma(part, part, t_send, t_recv.at[j], xdev).wait_recv()

    def stored(e):
        if e < blocks_own:
            return e // n_here * per_core + e % n_here
        e -= blocks_own
        return e // n_halo * per_core + n_here + e % n_halo

    ones = jnp.ones((16, 2 * tile), bf16)

    def scores_of(j, pair, keys_at):
        q_pair = qbuf[block(j), pair * pw : (pair + 1) * pw]
        zero = jnp.zeros_like(q_pair)
        wide = jnp.concatenate(
            [jnp.where(low_half, q_pair, zero), jnp.where(low_half, zero, q_pair)], axis=0
        )
        top = jnp.full((8, 2 * tile), NEG_FILL, f32)
        for n, e in enumerate(keys_at):
            bias = bias_ref[j, e * tile : (e + 1) * tile]
            scores = lax.dot_general(kv[stored(e), pair], wide, NT, preferred_element_type=f32)
            scores = scores + jnp.concatenate([bias, bias], axis=1)
            s_ref[pair, n * tile : (n + 1) * tile] = scores
            top = jnp.maximum(top, jnp.max(scores.reshape(tile // 8, 8, 2 * tile), axis=0))
        return jnp.max(top, axis=0, keepdims=True)

    def mixed_of(pair, keys_at, top):
        mixed = jnp.zeros((pw + 16, 2 * tile), f32)
        for n in range(0, len(keys_at), 2):
            p = jnp.exp2(s_ref[pair, n * tile : (n + 2) * tile] - top).astype(bf16)
            values = jnp.concatenate(
                [kv[stored(keys_at[n]), pairs + pair], kv[stored(keys_at[n + 1]), pairs + pair]],
                axis=1,
            )
            values = jnp.concatenate([values, ones], axis=0)
            mixed = mixed + jnp.dot(values, p, preferred_element_type=f32)
        heads = jnp.concatenate([mixed[:HD, :tile], mixed[HD:pw, tile:]], axis=0)
        return heads, mixed[pw : pw + 8]

    def both_heads(row):
        return jnp.concatenate(
            [
                jnp.broadcast_to(row[:, :tile], (HD, tile)),
                jnp.broadcast_to(row[:, tile:], (HD, tile)),
            ],
            axis=0,
        )

    late_keys = tuple(e for e in range(blocks_own) if e % n_here == last)
    early_keys = tuple(e for e in range(n_keys) if e not in late_keys)
    all_keys = early_keys + late_keys

    def attend_early(j):
        tops = [scores_of(j, pair, early_keys) for pair in range(pairs)]
        for pair in range(pairs):
            heads, sums = mixed_of(pair, early_keys, tops[pair])
            o_ref[pair] = heads
            l_ref[pair, :8] = sums
            l_ref[pair, 8:] = jnp.broadcast_to(tops[pair], (8, 2 * tile))

    def attend_late(j, pair):
        before = l_ref[pair, 8:9]
        top = jnp.maximum(scores_of(j, pair, late_keys), before)
        shrink = jnp.exp2(before - top)
        heads, sums = mixed_of(pair, late_keys, top)
        total = l_ref[pair, :1] * shrink + sums[:1]
        heads = o_ref[pair] * both_heads(shrink) + heads
        heads = heads * both_heads(1.0 / total)
        att[c * pairs + pair, block(j)] = heads.T.astype(bf16)
        t_copy(j, pair, 1).start()

    def attend_all(j, carry):
        with jax.named_scope("aall"):
            tops = [scores_of(j, pair, all_keys) for pair in range(pairs)]
            for pair in range(pairs):
                heads, sums = mixed_of(pair, all_keys, tops[pair])
                heads = heads * both_heads(1.0 / sums[:1])
                att[c * pairs + pair, block(j)] = heads.T.astype(bf16)
            t_copy(j, 0, pairs).start()
        return carry

    with jax.named_scope("kvw"):
        k_wait(0, last, 0)

        @pl.when(sib_halo)
        def _():
            k_wait(n_here, n_halo, 1)

    with jax.named_scope("early"):
        attend_early(0)
    with jax.named_scope("kvw2"):
        k_wait(last, 1, 2)
    for pair in range(pairs):
        with jax.named_scope("late"):
            attend_late(0, pair)
    lax.fori_loop(1, n_here, attend_all, 0)

    loaded(6)

    def p_copy(j, to):
        src = half_part.at[j, far + to]
        dev = {"chan": 1 - c, "sub": to}
        return rdma(src, from_x.at[j, s], p_send, x_recv.at[j], dev)

    def p_wait(j):
        part = from_x.at[j]
        rdma(part, part, p_send, x_recv.at[j], xdev).wait_recv()

    def d_copy(j):
        return rdma(full_part.at[j, sib], from_sib.at[j], d_send, d_recv.at[j], sdev)

    def ffn_block(j, carry):
        with jax.named_scope("tw"):
            t_wait(j)
        at = block(j)
        mixed = jnp.concatenate([att[g, at] for g in range(2 * pairs)], axis=1)
        after = full_rows(at) + jnp.dot(mixed, wo[...], preferred_element_type=f32)
        normed_two = norm(after, 1).astype(bf16)
        hidden = gelu_tanh(
            lax.dot_general(normed_two, fin[...], NT, preferred_element_type=f32)
        ).astype(bf16)
        part = jnp.dot(hidden, fout[...], preferred_element_type=f32)
        for g in range(groups):
            half_part[j, g] = part[:, g * cols : (g + 1) * cols].astype(bf16)
        p_copy(j, 0).start()
        p_copy(j, 1).start()
        whole = part + after
        for g in range(groups):
            full_part[j, g] = whole[:, g * cols : (g + 1) * cols]
        d_copy(j).start()
        return carry

    with jax.named_scope("ffn"):
        lax.fori_loop(0, n_here, ffn_block, 0)

    in_block = lax.broadcasted_iota(jnp.int32, (tile, cols), 0)

    def finish(j, carry):
        with jax.named_scope("pw"):
            d_copy(j).wait_recv()
            p_wait(j)
        for core, kept in ((s, full_part[j, own]), (1 - s, from_sib[j])):
            base = core * half + j * tile
            summed = kept + from_x[j, core].astype(f32)
            done = jnp.where(base + in_block < live, summed, 0.0).astype(bf16)
            out_ref[pl.ds(pl.multiple_of(base, tile), tile)] = done
        return carry

    with jax.named_scope("finish"):
        lax.fori_loop(0, n_here, finish, 0)

    def sent(part, sem):
        rdma(part, part, sem, sem, sdev).wait_send()

    with jax.named_scope("endw"):
        sent(xq, x_send)
        sent(xq.at[own_half], a_send)
        sent(kv.at[pl.ds(s * per_core, n_here)], k_send.at[0])
        sent(att.at[pl.ds(c * pairs, pairs)], t_send)
        sent(half_part.at[:, pl.ds(far, 2)], p_send)
        sent(from_sib, d_send)

        @pl.when(has_up)
        def _():
            z_copy(1).wait_send()

        @pl.when(has_down)
        def _():
            z_copy(0).wait_send()

        @pl.when(has_halo)
        def _():
            sent(gx.at[pl.ds(c * 2, 2), halo_at], h_send)
            sent(kv.at[pl.ds(s * per_core + n_here, n_halo)], k_send.at[1])


def one_kernel(*args):
    (x, gains, shifts, wq, wk, wv, wo, fin, fout, live, send, tk, bits) = args
    f32, bf16 = jnp.float32, jnp.bfloat16
    rows, cols = x.shape
    width = gains.shape[1]
    groups = lax.axis_size("chan") * lax.axis_size("sub")
    halo = send.shape[-1]
    tile = bits.shape[-1]
    slots = tk.shape[1]
    ext = rows + 2 * halo
    head_cols = wq.shape[1]
    half = rows // 2
    pairs = head_cols // (2 * HD)
    n_here = half // tile
    n_halo = halo // tile
    vmem = pltpu.VMEM
    dma = pltpu.SemaphoreType.DMA
    in_any = pl.BlockSpec(memory_space=pl.ANY)
    return pl.pallas_call(
        layer_kernel,
        out_shape=pltpu.VMEM(x.shape, bf16),
        in_specs=[in_any] * 13,
        out_specs=pl.BlockSpec(memory_space=pltpu.VMEM),
        scratch_shapes=[
            vmem(x.shape, bf16),
            vmem((groups, half + halo, cols), bf16),
            vmem((2, halo, cols), bf16),
            vmem((ext // tile, 2 * pairs, tile, 2 * HD), bf16),
            vmem((head_cols, width), bf16),
            vmem((half, head_cols), bf16),
            vmem((n_here, ext, tile), f32),
            vmem((pairs, ext, 2 * tile), f32),
            vmem((pairs, 2 * HD, tile), f32),
            vmem((pairs, 16, 2 * tile), f32),
            vmem((2 * pairs, half, 2 * HD), bf16),
            vmem((n_here, groups, tile, cols), f32),
            vmem((n_here, groups, tile, cols), bf16),
            vmem((n_here, tile, cols), f32),
            vmem((n_here, 2, tile, cols), bf16),
            vmem((width, 3 * head_cols), bf16),
            vmem((2 * fin.shape[0] + wo.shape[0], width), bf16),
            vmem((2 * gains.shape[0], width), f32),
            vmem(send.shape, jnp.int32),
            vmem(bits.shape, jnp.int32),
            pltpu.SMEM(live.shape, jnp.int32),
            pltpu.SMEM(tk.shape, jnp.int32),
            dma((7,)),
            dma((2,)),
            dma,
            dma,
            dma,
            dma((n_here,)),
            dma((2,)),
            dma,
            dma,
            dma((n_halo,)),
            dma((2,)),
            dma((3,)),
            dma,
            dma((n_here,)),
            dma,
            dma,
            dma((n_here,)),
        ],
        compiler_params=pltpu.CompilerParams(collective_id=0, has_side_effects=True),
    )(*args)


def on_any_device(*args):
    two_by_two = lax.axis_size("chan") == 2 and lax.axis_size("sub") == 2
    cols, head_cols = args[0].shape[1], args[3].shape[1]
    tile, halo = args[12].shape[-1], args[10].shape[-1]
    rows_fit = args[0].shape[0] % (4 * tile) == 0 and halo % (2 * tile) == 0
    few_slots = args[11].shape[1] < 16 and args[12].shape[-2] * 32 == tile and tile == cols
    if two_by_two and cols % 128 == 0 and head_cols % (2 * HD) == 0 and rows_fit and few_slots:
        return one_kernel(*args)
    return on_device(*args)


def solution(mesh):
    in_specs = (
        P(("ens", "space"), ("chan", "sub")),
        P(),
        P(),
        P(None, "chan"),
        P(None, "chan"),
        P(None, "chan"),
        P(),
        P("chan", None),
        P("chan", None),
        P("space"),
        P("space", None, None),
        P("space", None),
        P("space", None, None, None),
    )
    out_specs = P(("ens", "space"), ("chan", "sub"))
    return jax.shard_map(
        on_any_device, mesh=mesh, in_specs=in_specs, out_specs=out_specs, check_vma=False
    )
```

```python
import math

import jax
import jax.numpy as jnp
from jax import lax
from jax.experimental import pallas as pl
from jax.experimental.pallas import tpu as pltpu
from jax.sharding import PartitionSpec as P

HD = 64


NORM_EPS = 1e-05
NEG_FILL = -1e30


def padded_2(array, sides, width):
    for axis, dim in sides:
        size, length = (lax.axis_size(axis), array.shape[dim])
        up = [(i, (i + 1) % size) for i in range(size - 1)]
        down = [(j, i) for i, j in up]
        last = lax.slice_in_dim(array, length - width, length, axis=dim)
        leading = lax.slice_in_dim(array, 0, width, axis=dim)
        before = lax.ppermute(last, axis, up)
        after = lax.ppermute(leading, axis, down)
        array = jnp.concatenate([before, array, after], axis=dim)
    return array


def normalize_rows(source, gain_row, shift_row):
    row_mean = jnp.mean(source, axis=-1, keepdims=True)
    spread = jnp.mean(source * source, axis=-1, keepdims=True) - row_mean * row_mean
    return (source - row_mean) * lax.rsqrt(spread + NORM_EPS) * gain_row + shift_row


def unpack_allowed(key_bits, key_ids, live_count, tile_size, blocks_own):
    shifts = jnp.arange(32, dtype=jnp.int32)
    expanded = jnp.right_shift(key_bits[..., None, :], shifts[:, None]) & 1
    lead_shape = key_bits.shape[:-2]
    expanded = expanded.reshape(lead_shape + (tile_size, tile_size))
    key_index = key_ids[..., None] * tile_size + jnp.arange(tile_size, dtype=jnp.int32)
    key_live = (key_ids[..., None] >= blocks_own) | (key_index < live_count)
    slot_count = key_ids.shape[-1]
    slot_first = jnp.arange(slot_count, dtype=jnp.int32)[:, None, None] == 0
    diagonal = (
        jnp.arange(tile_size, dtype=jnp.int32)[:, None]
        == jnp.arange(tile_size, dtype=jnp.int32)[None, :]
    )
    own_bit = slot_first & diagonal[None]
    return (expanded == 1) & (key_live[..., None] | own_bit)


def hidden_term(rows, in_piece, out_piece):
    hidden = jax.nn.gelu(
        lax.dot_general(
            rows, in_piece, (((1,), (1,)), ((), ())), preferred_element_type=jnp.float32
        )
    ).astype(jnp.bfloat16)
    return jnp.dot(hidden, out_piece, preferred_element_type=jnp.float32)


def on_device(
    node_state,
    norm_gains,
    norm_shifts,
    query_weight,
    key_weight,
    value_weight,
    out_weight,
    ffn_in,
    ffn_out,
    live_counts,
    send_rows,
    tile_keys,
    tile_bits,
):
    n_chan = lax.axis_size("chan")
    n_sub = lax.axis_size("sub")
    groups = n_chan * n_sub
    chan_at = lax.axis_index("chan")
    sub_at = lax.axis_index("sub")
    node_rank = chan_at * n_sub + sub_at
    node_count = node_state.shape[0]
    tile_size = tile_bits.shape[-1]
    word_count = tile_bits.shape[-2]
    slot_count = tile_keys.shape[1]
    blocks_own = tile_keys.shape[0]
    per_rank = node_count // groups
    head_cols = query_weight.shape[1]
    heads_here = head_cols // HD
    halo_rows = send_rows.shape[-1]
    live_count = live_counts[0]

    def own_half(source):
        step_rows = source.shape[0] // groups
        shaped = source.reshape((n_chan, n_sub, step_rows) + source.shape[1:])
        picked = lax.dynamic_index_in_dim(shaped, sub_at, 1, keepdims=False)
        return picked.reshape((n_chan * step_rows,) + source.shape[1:])

    node_rows = lax.all_to_all(node_state, ("chan", "sub"), split_axis=0, concat_axis=1, tiled=True)
    pair_weight = jnp.concatenate([key_weight, value_weight], axis=1)
    gathered = lax.all_gather(node_state, ("chan", "sub"), axis=1, tiled=True)
    normed = normalize_rows(gathered.astype(jnp.float32), norm_gains[0], norm_shifts[0]).astype(
        jnp.bfloat16
    )
    key_values = jnp.dot(normed, pair_weight, preferred_element_type=jnp.float32).astype(
        jnp.bfloat16
    )
    queries = jnp.dot(own_half(normed), query_weight, preferred_element_type=jnp.float32).astype(
        jnp.bfloat16
    )
    send_list = send_rows.reshape(2 * halo_rows)
    outgoing = jnp.take(key_values, send_list, axis=0)
    padded = padded_2(outgoing, (("space", 0),), halo_rows)
    extended = jnp.concatenate([key_values, padded[:halo_rows], padded[-halo_rows:]], axis=0)
    key_blocks = extended.reshape(-1, tile_size, 2 * head_cols)
    key_ids = own_half(tile_keys)
    key_bits = own_half(tile_bits)
    block_total = key_ids.shape[0]
    per_round = math.gcd(block_total, 4)
    rounds = block_total // per_round
    score_scale = 1.0 / math.sqrt(HD)

    def attend(inputs):
        q_part, id_part, bit_part = inputs
        chosen = key_blocks[id_part]
        keys_part = chosen[..., :head_cols].reshape(
            per_round, slot_count, tile_size, heads_here, HD
        )
        values_part = chosen[..., head_cols:].reshape(
            per_round, slot_count, tile_size, heads_here, HD
        )
        scores = (
            jnp.einsum("grhd,gtkhd->ghrtk", q_part, keys_part, preferred_element_type=jnp.float32)
            * score_scale
        )
        allowed = unpack_allowed(bit_part, id_part, live_count, tile_size, blocks_own)
        allowed = jnp.transpose(allowed, (0, 3, 1, 2))[:, None]
        masked = jnp.where(allowed, scores, NEG_FILL)
        row_max = jnp.max(masked, axis=(3, 4), keepdims=True)
        weights = jnp.where(allowed, jnp.exp(scores - row_max), 0.0)
        row_total = jnp.sum(weights, axis=(3, 4))
        mixed_heads = jnp.einsum(
            "ghrtk,gtkhd->grhd",
            weights.astype(jnp.bfloat16),
            values_part,
            preferred_element_type=jnp.float32,
        )
        mixed_heads = mixed_heads / jnp.transpose(row_total, (0, 2, 1))[..., None]
        return mixed_heads.astype(jnp.bfloat16).reshape(per_round * tile_size, head_cols)

    query_groups = queries.reshape(rounds, per_round, tile_size, heads_here, HD)
    attended = lax.map(
        attend,
        (
            query_groups,
            key_ids.reshape(rounds, per_round, slot_count),
            key_bits.reshape(rounds, per_round, slot_count, word_count, tile_size),
        ),
    )
    mixed_rows = jnp.dot(
        lax.all_to_all(
            attended.reshape(n_chan, per_rank, head_cols),
            "chan",
            split_axis=0,
            concat_axis=2,
            tiled=True,
        )[0],
        out_weight,
        preferred_element_type=jnp.float32,
    )
    after_attn = node_rows.astype(jnp.float32) + mixed_rows
    normed_two = normalize_rows(after_attn, norm_gains[1], norm_shifts[1]).astype(jnp.bfloat16)
    all_rows = lax.all_gather(normed_two, "chan", axis=0, tiled=True)
    update = lax.psum_scatter(
        hidden_term(all_rows, ffn_in, ffn_out).astype(jnp.bfloat16),
        "chan",
        scatter_dimension=0,
        tiled=True,
    ).astype(jnp.float32)
    position = node_rank * per_rank + jnp.arange(per_rank, dtype=jnp.int32)
    result = jnp.where((position < live_count)[:, None], after_attn + update, 0.0).astype(
        jnp.bfloat16
    )
    return lax.all_to_all(result, ("chan", "sub"), split_axis=1, concat_axis=0, tiled=True)


MESH = pl.DeviceIdType.MESH
LOG2E = 1.4426950408889634
NT = (((1,), (1,)), ((), ()))


def gelu_tanh(u):
    inner = 0.7978845608028654 * (u + 0.044715 * (u * u * u))
    return 0.5 * u * (1.0 + jnp.tanh(inner))


def layer_kernel(
    x_hbm,
    gains_hbm,
    shifts_hbm,
    wq_hbm,
    wk_hbm,
    wv_hbm,
    wo_hbm,
    fin_hbm,
    fout_hbm,
    live_hbm,
    send_hbm,
    tk_hbm,
    bits_hbm,
    out_ref,
    xq,
    gx,
    hsend,
    kv,
    wvt,
    qbuf,
    bias_ref,
    s_ref,
    o_ref,
    l_ref,
    att,
    full_part,
    half_part,
    from_sib,
    from_x,
    proj_w,
    ffn_w,
    norm_ref,
    send_ref,
    bits_ref,
    live_ref,
    tk_ref,
    w_sem,
    loc_sem,
    a_send,
    a_recv,
    x_send,
    x_recv,
    z_send,
    z_recv,
    h_send,
    h_recv,
    k_send,
    k_recv,
    t_send,
    t_recv,
    p_send,
    d_send,
):
    f32, bf16 = jnp.float32, jnp.bfloat16
    rows, cols = x_hbm.shape
    groups = gx.shape[0]
    tile = bits_hbm.shape[-1]
    words = bits_hbm.shape[-2]
    slots = tk_ref.shape[1]
    blocks_own = tk_ref.shape[0]
    halo = send_hbm.shape[-1]
    width, head_cols = wv_hbm.shape
    hidden_here = fin_hbm.shape[0]
    pw = 2 * HD
    pairs = head_cols // pw
    half = rows // 2
    n_here = half // tile
    n_halo = halo // tile
    n_keys = blocks_own + 2 * n_halo

    c = lax.axis_index("chan")
    s = lax.axis_index("sub")
    z = lax.axis_index("space")
    nz = lax.axis_size("space")
    own = c * 2 + s
    sib = c * 2 + 1 - s
    far = (1 - c) * 2
    xdev = {"chan": 1 - c}
    sdev = {"sub": 1 - s}
    has_up = z < nz - 1
    has_down = z > 0
    has_halo = jnp.where(s == 0, z, nz - 1 - z) > 0
    sib_halo = jnp.where(s == 0, nz - 1 - z, z) > 0
    per_core = n_here + n_halo
    last = n_here - 1

    own_half = pl.ds(pl.multiple_of(s * half, half), half)
    sib_half = pl.ds(pl.multiple_of((1 - s) * half, half), half)
    local = pltpu.make_async_copy(x_hbm, xq, loc_sem.at[0])
    local_own = pltpu.make_async_copy(x_hbm.at[own_half], gx.at[own, pl.ds(0, half)], loc_sem.at[1])
    fin = ffn_w.at[pl.ds(0, hidden_here)]
    fout = ffn_w.at[pl.ds(hidden_here, hidden_here)]
    wo = ffn_w.at[pl.ds(2 * hidden_here, width)]
    n_norms = gains_hbm.shape[0]
    loads = (
        (send_hbm, send_ref, 0),
        (tk_hbm, tk_ref, 1),
        (live_hbm, live_ref, 2),
        (bits_hbm, bits_ref, 3),
        (wv_hbm, proj_w.at[:, pl.ds(2 * head_cols, head_cols)], 4),
        (gains_hbm, norm_ref.at[pl.ds(0, n_norms)], 5),
        (shifts_hbm, norm_ref.at[pl.ds(n_norms, n_norms)], 5),
        (wk_hbm, proj_w.at[:, pl.ds(0, head_cols)], 4),
        (wq_hbm, proj_w.at[:, pl.ds(head_cols, head_cols)], 4),
        (wo_hbm, wo, 6),
        (fin_hbm, fin, 6),
        (fout_hbm, fout, 6),
    )
    landed = (send_ref, tk_ref, live_ref, bits_ref, proj_w, norm_ref, ffn_w)

    def loaded(i):
        pltpu.make_async_copy(landed[i], landed[i], w_sem.at[i]).wait()


    barrier = pltpu.get_barrier_semaphore()

    def greet(dev):
        pl.semaphore_signal(barrier, inc=1, device_id=dev, device_id_type=MESH)

    greet(xdev)
    greet({"chan": 1 - c, "sub": 1 - s})
    greet(sdev)

    @pl.when(has_halo)
    def _():
        feeder = z - 1 + 2 * s
        greet({"space": feeder})
        greet({"space": feeder, "sub": 1 - s})

    local.start()
    local_own.start()
    for a, b, i in loads:
        pltpu.make_async_copy(a, b, w_sem.at[i]).start()
    with jax.named_scope("barrierw"):
        pl.semaphore_wait(barrier, 3 + jnp.where(has_up, 1, 0) + jnp.where(has_down, 1, 0))
    with jax.named_scope("localw"):
        local.wait()

    def rdma(src, dst, ss, rs, dev):
        return pltpu.make_async_remote_copy(
            src_ref=src, dst_ref=dst, send_sem=ss, recv_sem=rs, device_id=dev, device_id_type=MESH
        )

    def block(i):
        return pl.ds(pl.multiple_of(i * tile, tile), tile)

    def a_copy():
        return rdma(xq.at[sib_half], gx.at[own, pl.ds(0, half)], a_send, a_recv, sdev)

    def a_wait():
        part = gx.at[sib, pl.ds(0, half)]
        rdma(part, part, a_send, a_recv, sdev).wait_recv()

    def x_copy(i, to):
        src = xq.at[pl.ds(to * half + i * tile, tile)]
        dev = {"chan": 1 - c, "sub": to}
        return rdma(src, gx.at[own, block(i)], x_send, x_recv.at[i], dev)

    def x_wait(i):
        part = gx.at[pl.ds(far, 2), block(i)]
        rdma(part, part, x_send, x_recv.at[i], xdev).wait_recv()

    halo_at = pl.ds(half, halo)

    def z_copy(side):
        if side == 1:
            dev = {"space": z + 1, "sub": 0}
        else:
            dev = {"space": z - 1, "sub": 1}
        return rdma(hsend.at[side], gx.at[own, halo_at], z_send.at[side], z_recv, dev)

    def z_wait():
        part = gx.at[pl.ds(c * 2, 2), halo_at]
        rdma(part, part, z_send.at[0], z_recv, sdev).wait_recv()

    def h_copy(k):
        part = gx.at[pl.ds(c * 2, 2), pl.ds(half + k * tile, tile)]
        return rdma(part, part, h_send, h_recv.at[k], xdev)

    def h_wait(k):
        part = gx.at[pl.ds(far, 2), pl.ds(half + k * tile, tile)]
        rdma(part, part, h_send, h_recv.at[k], xdev).wait_recv()

    for i in range(last):
        x_copy(i, 0).start()
        x_copy(i, 1).start()
    a_copy().start()
    loaded(0)

    with jax.named_scope("onehot"):
        lanes = lax.broadcasted_iota(jnp.int32, (halo, tile), 1)
        for side in range(2):
            wanted = jnp.broadcast_to(send_ref[0, side : side + 1, :], (tile, halo)).T
            picks = jnp.concatenate(
                [(wanted == lanes + k * tile).astype(f32).astype(bf16) for k in range(rows // tile)],
                axis=1,
            )
            hsend[side] = jnp.dot(picks, xq[...], preferred_element_type=f32).astype(bf16)

    @pl.when(has_up)
    def _():
        z_copy(1).start()

    @pl.when(has_down)
    def _():
        z_copy(0).start()

    for core, there in ((s, has_halo), (1 - s, sib_halo)):

        @pl.when(jnp.logical_not(there))
        def _():
            empty = jnp.zeros((n_halo, 2 * pairs, tile, pw), bf16)
            kv[pl.ds(core * per_core + n_here, n_halo)] = empty

    for i in range(1, 5):
        loaded(i)
    wvt[...] = proj_w[:, 2 * head_cols :].astype(f32).T.astype(bf16)

    live = live_ref[0]
    word_rows = tile // words
    low_half = lax.broadcasted_iota(jnp.int32, (tile, pw), 1) < HD
    sub_row = lax.broadcasted_iota(jnp.int32, (8, tile), 0)
    phase = sub_row % 4
    high_nibble = sub_row // 4 * 4
    lane = lax.broadcasted_iota(jnp.int32, (words, tile), 1)
    first_key = lax.broadcasted_iota(jnp.int32, (words, tile), 0) * word_rows
    own_bit = jnp.where(
        lane // word_rows * word_rows == first_key,
        jnp.left_shift(jnp.ones_like(lane), lane % word_rows),
        0,
    )

    def mask_block(j, carry):
        b = s * n_here + j
        ids = [tk_ref[b, t] for t in range(slots)]
        spread = []
        for t in range(slots):
            limit = jnp.where(ids[t] >= blocks_own, tile, live - ids[t] * tile)
            count = jnp.clip(limit - first_key, 0, word_rows)
            some = jnp.left_shift(jnp.ones_like(count), jnp.minimum(count, word_rows - 1)) - 1
            good = jnp.where(count >= word_rows, -1, some)
            if t == 0:
                good = good | own_bit
            kept = bits_ref[b, t] & good
            spread.append(
                [
                    jnp.right_shift(jnp.broadcast_to(kept[w : w + 1, :], (8, tile)), phase)
                    & 0x11111111
                    for w in range(words)
                ]
            )
        for e in range(n_keys):
            picks = [jnp.where(ids[t] == e, -1, 0) for t in range(slots)]
            for w in range(words):
                total = spread[0][w] & picks[0]
                for t in range(1, slots):
                    total = total + (spread[t][w] & picks[t])
                for m in range(word_rows // 8):
                    times = jnp.right_shift(total, high_nibble + 8 * m) & 15
                    at = e * tile + w * word_rows + m * 8
                    bias_ref[j, at : at + 8] = jnp.maximum(jnp.log2(times.astype(f32)), NEG_FILL)
        return carry

    with jax.named_scope("mask"):
        lax.fori_loop(0, n_here, mask_block, 0)

    def full_rows(at):
        return jnp.concatenate([gx[g, at] for g in range(groups)], axis=1).astype(f32)

    def norm(v, which):
        mean = jnp.mean(v, axis=-1, keepdims=True)
        spread = jnp.mean(v * v, axis=-1, keepdims=True) - mean * mean
        scaled = (v - mean) * lax.rsqrt(spread + NORM_EPS)
        gain, shift = norm_ref[which : which + 1, :], norm_ref[n_norms + which : n_norms + which + 1, :]
        return scaled * gain + shift

    scale = LOG2E / math.sqrt(HD)

    def kv_copy(i, first, count, kind):
        part = kv.at[s * per_core + i, pl.ds(first, count)]
        return rdma(part, part, k_send.at[kind % 2], k_recv.at[kind], sdev)

    def k_wait(first, count, kind):
        part = kv.at[pl.ds((1 - s) * per_core + first, count)]
        rdma(part, part, k_send.at[0], k_recv.at[kind], sdev).wait_recv()

    def half_wait(i, first, kind):
        part = kv.at[(1 - s) * per_core + i, pl.ds(first, pairs)]
        rdma(part, part, k_send.at[0], k_recv.at[kind], sdev).wait_recv()

    def project(i, kind):
        normed = norm(full_rows(block(i)), 0).astype(bf16)
        to = s * per_core + i
        wanted = (2 if kind == 0 else 1) * head_cols
        both = jnp.dot(normed, proj_w[:, :wanted], preferred_element_type=f32)
        for pair in range(pairs):
            kv[to, pair] = both[:, pair * pw : (pair + 1) * pw].astype(bf16)
        if kind == 2:
            kv_copy(i, 0, pairs, 2).start()
        values = lax.dot_general(wvt[...], normed, NT, preferred_element_type=f32)
        for pair in range(pairs):
            kv[to, pairs + pair] = values[pair * pw : (pair + 1) * pw].astype(bf16)
        if kind == 2:
            kv_copy(i, pairs, pairs, 4).start()
        else:
            kv_copy(i, 0, 2 * pairs, kind).start()
        if kind == 0:
            queries = both[:, head_cols:]
        elif kind == 2:
            queries = jnp.dot(
                normed, proj_w[:, head_cols : 2 * head_cols], preferred_element_type=f32
            )
        if kind != 1:
            qbuf[block(i)] = (queries * scale).astype(bf16)

    loaded(5)
    local_own.wait()
    with jax.named_scope("aw"):
        a_wait()

    def own_step(i, carry):
        with jax.named_scope("xw"):
            x_wait(i)
        with jax.named_scope("proj"):
            project(i, 0)
        return carry

    lax.fori_loop(0, 1, own_step, 0)

    with jax.named_scope("zw"):

        @pl.when(has_halo)
        def _():
            z_wait()
            for k in range(n_halo):
                h_copy(k).start()

    x_copy(last, 0).start()
    x_copy(last, 1).start()
    lax.fori_loop(1, last, own_step, 0)

    def t_copy(j, first, count):
        part = att.at[pl.ds(c * pairs + first, count), block(j)]
        return rdma(part, part, t_send, t_recv.at[j], xdev)

    def t_wait(j):
        part = att.at[pl.ds((1 - c) * pairs, pairs), block(j)]
        rdma(part, part, t_send, t_recv.at[j], xdev).wait_recv()

    def stored(e):
        if e < blocks_own:
            return e // n_here * per_core + e % n_here
        e -= blocks_own
        return e // n_halo * per_core + n_here + e % n_halo

    ones = jnp.ones((16, 2 * tile), bf16)

    def scores_of(j, pair, keys_at):
        q_pair = qbuf[block(j), pair * pw : (pair + 1) * pw]
        zero = jnp.zeros_like(q_pair)
        wide = jnp.concatenate(
            [jnp.where(low_half, q_pair, zero), jnp.where(low_half, zero, q_pair)], axis=0
        )
        top = jnp.full((8, 2 * tile), NEG_FILL, f32)
        for n, e in enumerate(keys_at):
            bias = bias_ref[j, e * tile : (e + 1) * tile]
            scores = lax.dot_general(kv[stored(e), pair], wide, NT, preferred_element_type=f32)
            scores = scores + jnp.concatenate([bias, bias], axis=1)
            s_ref[pair, n * tile : (n + 1) * tile] = scores
            top = jnp.maximum(top, jnp.max(scores.reshape(tile // 8, 8, 2 * tile), axis=0))
        return jnp.max(top, axis=0, keepdims=True)

    def mixed_of(pair, keys_at, top):
        mixed = jnp.zeros((pw + 16, 2 * tile), f32)
        for n in range(0, len(keys_at), 2):
            p = jnp.exp2(s_ref[pair, n * tile : (n + 2) * tile] - top).astype(bf16)
            values = jnp.concatenate(
                [kv[stored(keys_at[n]), pairs + pair], kv[stored(keys_at[n + 1]), pairs + pair]],
                axis=1,
            )
            values = jnp.concatenate([values, ones], axis=0)
            mixed = mixed + jnp.dot(values, p, preferred_element_type=f32)
        heads = jnp.concatenate([mixed[:HD, :tile], mixed[HD:pw, tile:]], axis=0)
        return heads, mixed[pw : pw + 8]

    def both_heads(row):
        return jnp.concatenate(
            [
                jnp.broadcast_to(row[:, :tile], (HD, tile)),
                jnp.broadcast_to(row[:, tile:], (HD, tile)),
            ],
            axis=0,
        )

    late_keys = tuple(e for e in range(blocks_own) if e % n_here == last)
    early_keys = tuple(e for e in range(blocks_own) if e not in late_keys)
    halo_keys = tuple(range(blocks_own, n_keys))
    all_keys = early_keys + halo_keys + late_keys

    def attend_some(j, keys_at, first):
        tops = [scores_of(j, pair, keys_at) for pair in range(pairs)]
        for pair in range(pairs):
            top = tops[pair]
            if not first:
                before = l_ref[pair, 8:9]
                top = jnp.maximum(top, before)
                shrink = jnp.exp2(before - top)
            heads, sums = mixed_of(pair, keys_at, top)
            if not first:
                heads = o_ref[pair] * both_heads(shrink) + heads
                sums = l_ref[pair, :8] * shrink + sums
            o_ref[pair] = heads
            l_ref[pair, :8] = sums
            l_ref[pair, 8:] = jnp.broadcast_to(top, (8, 2 * tile))

    def attend_late(j, pair):
        before = l_ref[pair, 8:9]
        top = jnp.maximum(scores_of(j, pair, late_keys), before)
        shrink = jnp.exp2(before - top)
        if pair == 0:
            half_wait(last, pairs, 4)
        heads, sums = mixed_of(pair, late_keys, top)
        total = l_ref[pair, :1] * shrink + sums[:1]
        heads = o_ref[pair] * both_heads(shrink) + heads
        heads = heads * both_heads(1.0 / total)
        att[c * pairs + pair, block(j)] = heads.T.astype(bf16)

    def finish_pair(j, pair, top):
        heads, sums = mixed_of(pair, all_keys, top)
        heads = heads * both_heads(1.0 / sums[:1])
        att[c * pairs + pair, block(j)] = heads.T.astype(bf16)

    def attend_all(j, top):
        with jax.named_scope("aall"):
            for pair in range(pairs):
                finish_pair(j, pair, top)
                following = j if pair + 1 < pairs else j + 1
                top = scores_of(following, (pair + 1) % pairs, all_keys)
                t_copy(j, pair, 1).start()
        return top

    def attend_end(j, top):
        for pair in range(pairs):
            finish_pair(j, pair, top)
            if pair + 1 < pairs:
                top = scores_of(j, pair + 1, all_keys)
            t_copy(j, pair, 1).start()

    def halo_step(k):
        @pl.when(has_halo)
        def _():
            with jax.named_scope("hw"):
                h_wait(k)
            with jax.named_scope("hproj"):
                project(n_here + k, 1)

    halo_step(0)
    with jax.named_scope("kvw"):
        k_wait(0, last, 0)
    with jax.named_scope("early"):
        attend_some(0, early_keys, True)
    for k in range(1, n_halo):
        halo_step(k)
    with jax.named_scope("xw"):
        x_wait(last)
    with jax.named_scope("proj"):
        project(last, 2)
    with jax.named_scope("kvw1"):

        @pl.when(sib_halo)
        def _():
            k_wait(n_here, n_halo, 1)

    with jax.named_scope("ehalo"):
        attend_some(0, halo_keys, False)
    with jax.named_scope("kvw2"):
        half_wait(last, 0, 2)
    for pair in range(pairs):
        with jax.named_scope("late"):
            attend_late(0, pair)
            if pair + 1 == pairs:
                top = scores_of(1, 0, all_keys)
            t_copy(0, pair, 1).start()
    top = lax.fori_loop(1, last, attend_all, top)
    with jax.named_scope("aend"):
        attend_end(last, top)

    loaded(6)
    landed_part = full_part.at[:, pl.ds(0, 2)]

    def p_copy(j, to):
        src = half_part.at[j, far + to]
        dev = {"chan": 1 - c, "sub": to}
        return rdma(src, from_x.at[j, s], p_send, x_recv.at[j], dev)

    def p_wait(j):
        part = landed_part.at[j]
        rdma(part, part, p_send, x_recv.at[j], xdev).wait_recv()

    def d_copy(j):
        return rdma(full_part.at[j, sib], from_sib.at[j], d_send, x_recv.at[j], sdev)

    def ffn_block(j, carry):
        with jax.named_scope("tw"):
            t_wait(j)
        at = block(j)
        mixed = jnp.concatenate([att[g, at] for g in range(2 * pairs)], axis=1)
        after = full_rows(at) + jnp.dot(mixed, wo[...], preferred_element_type=f32)
        normed_two = norm(after, 1).astype(bf16)
        hidden = gelu_tanh(
            lax.dot_general(normed_two, fin[...], NT, preferred_element_type=f32)
        ).astype(bf16)
        part = jnp.dot(hidden, fout[...], preferred_element_type=f32)
        for g in range(groups):
            half_part[j, g] = part[:, g * cols : (g + 1) * cols].astype(bf16)
        p_copy(j, 0).start()
        p_copy(j, 1).start()
        whole = part + after
        for g in range(groups):
            full_part[j, g] = whole[:, g * cols : (g + 1) * cols]
        d_copy(j).start()
        return carry

    with jax.named_scope("ffn"):
        lax.fori_loop(0, n_here, ffn_block, 0)

    in_block = lax.broadcasted_iota(jnp.int32, (tile, cols), 0)

    def finish(j, carry):
        with jax.named_scope("pw"):
            p_wait(j)
        for core, kept in ((s, full_part[j, own]), (1 - s, from_sib[j])):
            base = core * half + j * tile
            summed = kept + from_x[j, core].astype(f32)
            done = jnp.where(base + in_block < live, summed, 0.0).astype(bf16)
            out_ref[pl.ds(pl.multiple_of(base, tile), tile)] = done
        return carry

    with jax.named_scope("finish"):
        lax.fori_loop(0, n_here, finish, 0)

    def sent(part, sem):
        rdma(part, part, sem, sem, sdev).wait_send()

    with jax.named_scope("endw"):
        sent(xq, x_send)
        sent(xq.at[own_half], a_send)
        sent(kv.at[pl.ds(s * per_core, n_here)], k_send.at[0])
        sent(att.at[pl.ds(c * pairs, pairs)], t_send)
        sent(half_part.at[:, pl.ds(far, 2)], p_send)
        sent(from_sib, d_send)

        @pl.when(has_up)
        def _():
            z_copy(1).wait_send()

        @pl.when(has_down)
        def _():
            z_copy(0).wait_send()

        @pl.when(has_halo)
        def _():
            sent(gx.at[pl.ds(c * 2, 2), halo_at], h_send)
            sent(kv.at[pl.ds(s * per_core + n_here, n_halo)], k_send.at[1])


def one_kernel(*args):
    (x, gains, shifts, wq, wk, wv, wo, fin, fout, live, send, tk, bits) = args
    f32, bf16 = jnp.float32, jnp.bfloat16
    rows, cols = x.shape
    width = gains.shape[1]
    groups = lax.axis_size("chan") * lax.axis_size("sub")
    halo = send.shape[-1]
    tile = bits.shape[-1]
    slots = tk.shape[1]
    ext = rows + 2 * halo
    head_cols = wq.shape[1]
    half = rows // 2
    pairs = head_cols // (2 * HD)
    n_here = half // tile
    n_halo = halo // tile
    vmem = pltpu.VMEM
    dma = pltpu.SemaphoreType.DMA
    in_any = pl.BlockSpec(memory_space=pl.ANY)
    return pl.pallas_call(
        layer_kernel,
        out_shape=pltpu.VMEM(x.shape, bf16),
        in_specs=[in_any] * 13,
        out_specs=pl.BlockSpec(memory_space=pltpu.VMEM),
        scratch_shapes=[
            vmem(x.shape, bf16),
            vmem((groups, half + halo, cols), bf16),
            vmem((2, halo, cols), bf16),
            vmem((ext // tile, 2 * pairs, tile, 2 * HD), bf16),
            vmem((head_cols, width), bf16),
            vmem((half, head_cols), bf16),
            vmem((n_here, ext, tile), f32),
            vmem((pairs, ext, 2 * tile), f32),
            vmem((pairs, 2 * HD, tile), f32),
            vmem((pairs, 16, 2 * tile), f32),
            vmem((2 * pairs, half, 2 * HD), bf16),
            vmem((n_here, groups, tile, cols), f32),
            vmem((n_here, groups, tile, cols), bf16),
            vmem((n_here, tile, cols), f32),
            vmem((n_here, 2, tile, cols), bf16),
            vmem((width, 3 * head_cols), bf16),
            vmem((2 * fin.shape[0] + wo.shape[0], width), bf16),
            vmem((2 * gains.shape[0], width), f32),
            vmem(send.shape, jnp.int32),
            vmem(bits.shape, jnp.int32),
            pltpu.SMEM(live.shape, jnp.int32),
            pltpu.SMEM(tk.shape, jnp.int32),
            dma((7,)),
            dma((2,)),
            dma,
            dma,
            dma,
            dma((n_here,)),
            dma((2,)),
            dma,
            dma,
            dma((n_halo,)),
            dma((2,)),
            dma((5,)),
            dma,
            dma((n_here,)),
            dma,
            dma,
        ],
        compiler_params=pltpu.CompilerParams(collective_id=0, has_side_effects=True),
    )(*args)


def on_any_device(*args):
    two_by_two = lax.axis_size("chan") == 2 and lax.axis_size("sub") == 2
    cols, head_cols = args[0].shape[1], args[3].shape[1]
    tile, halo = args[12].shape[-1], args[10].shape[-1]
    rows_fit = args[0].shape[0] % (4 * tile) == 0 and halo % (2 * tile) == 0
    few_slots = args[11].shape[1] < 16 and args[12].shape[-2] * 32 == tile and tile == cols
    if two_by_two and cols % 128 == 0 and head_cols % (2 * HD) == 0 and rows_fit and few_slots:
        return one_kernel(*args)
    return on_device(*args)


def solution(mesh):
    in_specs = (
        P(("ens", "space"), ("chan", "sub")),
        P(),
        P(),
        P(None, "chan"),
        P(None, "chan"),
        P(None, "chan"),
        P(),
        P("chan", None),
        P("chan", None),
        P("space"),
        P("space", None, None),
        P("space", None),
        P("space", None, None, None),
    )
    out_specs = P(("ens", "space"), ("chan", "sub"))
    return jax.shard_map(
        on_any_device, mesh=mesh, in_specs=in_specs, out_specs=out_specs, check_vma=False
    )
```
